32 devices in a mesh: rep: 4 (over x, core), grp: 8 (over z, y).
Axes of the slice: x: 2, y: 2, z: 4, core: 2. Of those that a mesh axis runs over, the one named last changes fastest.
Arguments:
- tokens: bfloat16 [8192, 2304], P(('rep', 'grp')), may hold values from -6 to 6
- norm_gain: float32 [2304], replicated, may hold values from 0.25 to 1.75
- key_weight: bfloat16 [2304, 1024], P('grp'), may hold values from -0.125 to 0.125
- key_grad: bfloat16 [8192, 1024], P(('rep', 'grp')), may hold values from -6 to 6
Outputs:
- token_grad: bfloat16 [8192, 2304], P(('rep', 'grp'))
- weight_grad: float32 [2304, 1024], P('grp', 'rep')
- gain_grad: float32 [2304], replicated
The draws below stay inside these ranges and needn't reach their ends.
All inputs are finite; a program needn't handle non-finite values.
Results may differ from the reference program's by a relative error of at most 0.023.
Values may be sent and summed in bfloat16 or wider, within the bound.
A program may use at most 64 MiB of HBM per device.

```python
import jax
import jax.numpy as jnp
from jax import lax

D = 2304
KV_HEADS = 8
HEAD_DIM = 128
KEYS = 1024
TOK_DEV = 256
TOKENS = 8192
N_REP = 4
N_GRP = 8


def block_levels(key, extent, pieces, low, largest):
    def one(axis_at, blocks):
        steps = jax.random.uniform(jax.random.fold_in(jax.random.fold_in(key, 6), axis_at), (blocks,), jnp.float32, low / len(pieces), largest / len(pieces))
        return jnp.repeat(jnp.exp(steps), extent[axis_at] // blocks).reshape((-1,) + (1,) * (len(extent) - axis_at - 1))

    loudness = one(*pieces[0])
    for cut in pieces[1:]:
        loudness = loudness * one(*cut)
    return loudness


def bell_draw(own_key, dims, spread, reach, shards=(), dtype=jnp.bfloat16):
    array = jax.random.normal(own_key, dims, jnp.float32) * spread
    if len(shards) > 0:
        array = block_levels(own_key, dims, shards, -0.22, 0.18) * array
    return jnp.clip(array, min=-reach, max=reach).astype(dtype)


def setup_inputs(seed: int = 0) -> dict:
    key_list = jax.random.split(jax.random.key(seed), 5)
    tokens = bell_draw(key_list[0], (TOKENS, D), 1.0, 6.0, ((0, 32),))
    norm_gain = jnp.clip(1.0 + 0.15 * jax.random.normal(key_list[1], (D,), jnp.float32), 0.25, 1.75)
    key_weight = bell_draw(key_list[2], (D, KEYS), D ** -0.5, 0.125, ((0, 8),))
    key_grad = bell_draw(key_list[3], (TOKENS, KEYS), 1.0, 6.0, ((0, 32),))
    return {"tokens": tokens, "norm_gain": norm_gain, "key_weight": key_weight, "key_grad": key_grad}


epsilon = 1e-06

def reference(tokens, norm_gain, key_weight, key_grad):
    grad_scale = (TOK_DEV * N_REP * N_GRP) ** (-0.5)
    blocks = tokens.reshape(N_REP * N_GRP, TOK_DEV, D)
    key_blocks = key_grad.reshape(N_REP * N_GRP, TOK_DEV, KV_HEADS * HEAD_DIM)

    def one_block(carry, inputs):
        running, gain_total = carry
        block_tokens, block_keys = inputs
        wide_tokens = block_tokens.astype(jnp.float32)
        inv_rms = lax.rsqrt(lax.optimization_barrier(jnp.mean(wide_tokens * wide_tokens, axis=1, keepdims=True)) + epsilon)
        normed = (wide_tokens * inv_rms * norm_gain).astype(jnp.bfloat16)
        partial_value = lax.dot_general(normed, block_keys, (((0,), (0,)), ((), ())), preferred_element_type=jnp.float32)
        rounded = lax.optimization_barrier(partial_value.astype(jnp.bfloat16)).astype(jnp.float32)
        d_normed = lax.dot_general(block_keys, key_weight, (((1,), (1,)), ((), ())), preferred_element_type=jnp.float32)
        gain_part = lax.optimization_barrier(jnp.sum(d_normed * wide_tokens * inv_rms, axis=0))
        scaled = d_normed * norm_gain
        inner_mean = lax.optimization_barrier(jnp.mean(scaled * wide_tokens, axis=1, keepdims=True))
        block_grad = (inv_rms * (scaled - wide_tokens * inv_rms * inv_rms * inner_mean)).astype(jnp.bfloat16)
        return ((running + rounded, gain_total + gain_part), block_grad)
    start = (jnp.zeros((D, KV_HEADS * HEAD_DIM), jnp.float32), jnp.zeros((D,), jnp.float32))
    (running, gain_total), grads = lax.scan(one_block, start, (blocks, key_blocks))
    token_grad = grads.reshape(N_REP * N_GRP * TOK_DEV, D)
    return (token_grad, running * grad_scale, gain_total * grad_scale)
```

```python
import functools

import jax
import jax.numpy as jnp
from jax import lax
from jax.experimental import pallas as pl
from jax.experimental.pallas import tpu as pltpu
from jax.sharding import PartitionSpec as P

epsilon = 1e-06
MESH = pl.DeviceIdType.MESH
LANES = 128


def flip(i, bits):
    bit = 1
    while bit <= bits:
        if bits & bit:
            i = i + bit * (1 - 2 * lax.rem(lax.div(i, bit), 2))
        bit *= 2
    return i


def kernel(
    n_z, grad_scale,
    tok_hbm, gain_hbm, w_ref, kg_hbm,
    tg_ref, wg_ref, gg_ref,
    tok_ref, gain_ref, kg_ref, load_sem, wfull, normed_t, dn, mine, give, take, in1, in2, in3, gsend, grecv,
    w_send, w_recv, c_send, c_recv, s1_send, s1_recv, s2_send, s2_recv, s3_send, s3_recv, g_send, g_recv,
):
    rep, grp = lax.axis_index("rep"), lax.axis_index("grp")
    x, c = lax.div(rep, 2), lax.rem(rep, 2)
    z, y = lax.div(grp, 2), lax.rem(grp, 2)
    rows, keys = w_ref.shape
    features = tok_ref.shape[1]
    cols = mine.shape[-1]
    peer_c = (2 * x + 1 - c, grp)
    peer_x = (2 * (1 - x) + c, grp)
    peer_cx = (2 * (1 - x) + 1 - c, grp)
    peer_y = (rep, 2 * z + 1 - y)
    peer_z = [None] + [(rep, 2 * flip(z, k) + y) for k in range(1, n_z)]
    group = [peer_y]
    for k in range(1, n_z):
        group += [peer_z[k], (rep, 2 * flip(z, k) + 1 - y)]

    def row_at(k, yy):
        g = 2 * flip(z, k) + (1 - y if yy else y)
        return pl.ds(pl.multiple_of(g * rows, 16), rows)

    loads = [
        pltpu.make_async_copy(src, dst, load_sem.at[n])
        for n, (src, dst) in enumerate(
            ((tok_hbm, tok_ref), (gain_hbm, gain_ref), (kg_hbm, kg_ref), (w_ref, wfull.at[row_at(0, 0), :]))
        )
    ]
    for load in loads:
        load.start()

    barrier = pltpu.get_barrier_semaphore()
    peers = [peer_c, peer_x, peer_cx] + group
    for peer in peers:
        pl.semaphore_signal(barrier, inc=1, device_id=peer, device_id_type=MESH)
    pl.semaphore_wait(barrier, len(peers))

    sends = []

    def send(src, dst, s_sem, r_sem, peer):
        copy = pltpu.make_async_remote_copy(
            src_ref=src, dst_ref=dst, send_sem=s_sem, recv_sem=r_sem, device_id=peer, device_id_type=MESH
        )
        copy.start()
        sends.append(copy)

    def arrived(dst, sem):
        pltpu.make_async_remote_copy(
            src_ref=dst, dst_ref=dst, send_sem=sem, recv_sem=sem, device_id=peer_c, device_id_type=MESH
        ).wait_recv()

    def col_at(xx, cc):
        r = 2 * (1 - x if xx else x) + (1 - c if cc else c)
        return pl.ds(pl.multiple_of(r * cols, LANES), cols)

    def piece(xx, cc, k, yy):
        return wfull.at[row_at(k, yy), col_at(xx, cc)]

    def got(xx, cc, k, yy):
        arrived(piece(xx, cc, k, yy), w_recv.at[xx, cc, k, yy])

    def w_fwd(axis, xx, k, yy):
        there = {0: (xx, 1, k, yy), 1: (1 - xx, 0, k, yy), 2: (xx, 0, k, 1 - yy)}[axis]
        peer = (peer_c, peer_x, peer_y)[axis]
        ref = piece(xx, 0, k, yy)
        send(ref, ref, w_send.at[axis, xx, k, yy], w_recv.at[there], peer)

    def own_to(axis, xx, k, peer):
        there = (xx, 0, 0, 1) if axis == 2 else (xx, 0, k, 0)
        send(
            w_ref.at[:, col_at(xx, 0)], piece(xx, 0, 0, 0), w_send.at[axis, xx, k, 0], w_recv.at[there], peer
        )

    own_to(2, 0, 0, peer_y)
    for k in range(1, n_z):
        own_to(3, 0, k, peer_z[k])
    own_to(2, 1, 0, peer_y)
    for k in range(1, n_z - 1):
        own_to(3, 1, k, peer_z[k])

    loads[0].wait()
    acc = None
    for j in range(features // LANES):
        t = tok_ref[:, j * LANES:(j + 1) * LANES].astype(jnp.float32)
        acc = t * t if acc is None else acc + t * t
    inv = lax.rsqrt(jnp.sum(acc, axis=1, keepdims=True) / features + epsilon)
    loads[1].wait()
    for j in range(features // LANES):
        at = slice(j * LANES, (j + 1) * LANES)
        t = tok_ref[:, at].astype(jnp.float32)
        normed_t[at, :] = (t * inv * gain_ref[at].reshape(1, -1)).T.astype(jnp.bfloat16)

    def partial(k):
        for cc in (1, 0):
            for yy in (0, 1):
                for xx in (0, 1):
                    block = jnp.dot(
                        normed_t[row_at(k, yy), :], kg_ref[:, col_at(xx, cc)], preferred_element_type=jnp.float32
                    ).astype(jnp.bfloat16)
                    (give if cc else mine)[k, yy, xx] = block
            if cc:
                send(give.at[k], take.at[k], c_send.at[k], c_recv.at[k], peer_c)

    def add(k, yy, xx, ref):
        mine[k, yy, xx] = (
            mine[k, yy, xx].astype(jnp.float32) + ref[...].astype(jnp.float32)
        ).astype(jnp.bfloat16)

    def x_first(k):
        return k % 2 == 1

    def core_in(k):
        arrived(take.at[k], c_recv.at[k])

    def stage1(k, slot):
        for other in (1, 0):
            yy, xx = (slot, other) if x_first(k) else (other, slot)
            add(k, yy, xx, take.at[k, yy, xx])
            if other:
                send(
                    mine.at[k, yy, xx], in1.at[k, slot], s1_send.at[k, slot], s1_recv.at[k, slot],
                    peer_x if x_first(k) else peer_y,
                )

    def stage2(k, slot):
        arrived(in1.at[k, slot], s1_recv.at[k, slot])
        yy, xx = (slot, 0) if x_first(k) else (0, slot)
        add(k, yy, xx, in1.at[k, slot])
        if slot:
            send(mine.at[k, yy, xx], in2.at[k], s2_send.at[k], s2_recv.at[k], peer_y if x_first(k) else peer_x)

    def stage3(k):
        arrived(in2.at[k], s2_recv.at[k])
        add(k, 0, 0, in2.at[k])
        send(mine.at[k, 0, 0], in3.at[k], s3_send.at[k], s3_recv.at[k], peer_z[k])

    def take_on(xx, k, yy, *axes):
        got(xx, 0, k, yy)
        for axis in axes + (0,):
            w_fwd(axis, xx, k, yy)

    loads[2].wait()
    partial(3)
    take_on(0, 1, 0, 2)
    partial(2)
    core_in(3)
    stage1(3, 1)
    stage1(3, 0)
    take_on(0, 2, 0, 2)
    core_in(2)
    stage1(2, 1)
    stage1(2, 0)
    take_on(0, 0, 1)
    take_on(0, 1, 1, 1)
    partial(1)
    partial(0)
    take_on(0, 2, 1, 1)
    stage2(3, 1)
    take_on(0, 3, 0, 1, 2)
    core_in(1)
    core_in(0)
    stage2(3, 0)
    take_on(1, 0, 1)
    take_on(1, 1, 0)
    stage2(2, 1)
    take_on(1, 1, 1)
    stage1(1, 1)
    stage1(0, 1)
    stage1(0, 0)
    take_on(1, 2, 1)
    take_on(0, 3, 1, 1)
    stage1(1, 0)
    take_on(1, 2, 0)
    stage2(2, 0)
    take_on(1, 3, 0)
    stage3(3)
    stage3(2)
    stage2(1, 1)
    stage2(0, 1)
    take_on(1, 3, 1)
    loads[3].wait()
    for k in range(n_z):
        for yy in (0, 1):
            for xx in (0, 1):
                if k or yy:
                    got(xx, 1, k, yy)

    wide = 2 * LANES
    inner = jnp.zeros((tok_ref.shape[0], LANES), jnp.float32)
    for j in range(features // wide):
        at = slice(j * wide, (j + 1) * wide)
        d = lax.dot_general(
            kg_ref[...], wfull[at, :], (((1,), (1,)), ((), ())), preferred_element_type=jnp.float32
        )
        dn[:, at] = d
        dt = d * tok_ref[:, at].astype(jnp.float32)
        gsend[0, :, at] = jnp.sum(dt * inv, axis=0, keepdims=True)
        scaled = dt * gain_ref[at].reshape(1, -1)
        inner = inner + scaled[:, :LANES] + scaled[:, LANES:]
    for n, peer in enumerate((peer_c, peer_x, peer_cx)):
        send(gsend.at[0], grecv.at[n], g_send.at[n], g_recv.at[n], peer)
    for k in (1, 0):
        stage2(k, 0)
    stage3(1)
    mean = jnp.sum(inner, axis=1, keepdims=True) / features
    pull = inv * inv * mean

    def token_grad(lo, hi):
        for j in range(lo, hi):
            at = slice(j * wide, (j + 1) * wide)
            t = tok_ref[:, at].astype(jnp.float32)
            tg_ref[:, at] = (inv * (dn[:, at] * gain_ref[at].reshape(1, -1) - t * pull)).astype(jnp.bfloat16)

    steps = features // wide
    token_grad(0, steps // 3)
    for n in range(3):
        arrived(grecv.at[n], g_recv.at[n])
    gsend[1] = (gsend[0] + grecv[0]) + (grecv[1] + grecv[2])
    for n, peer in enumerate(group):
        send(gsend.at[1], grecv.at[3 + n], g_send.at[3 + n], g_recv.at[3 + n], peer)
    token_grad(steps // 3, steps)

    arrived(in2.at[0], s2_recv.at[0])
    total = mine[0, 0, 0].astype(jnp.float32) + in2[0].astype(jnp.float32)
    for k in range(1, n_z):
        arrived(in3.at[k], s3_recv.at[k])
        total = total + in3[k].astype(jnp.float32)
    wg_ref[...] = total * grad_scale

    terms = [gsend[1]]
    for n in range(3, 3 + len(group)):
        arrived(grecv.at[n], g_recv.at[n])
        terms.append(grecv[n])
    while len(terms) > 1:
        terms = [terms[i] + terms[i + 1] for i in range(0, len(terms), 2)]
    total = terms[0] * grad_scale
    for j in range(features // LANES):
        at = slice(j * LANES, (j + 1) * LANES)
        gg_ref[at] = total[:, at].reshape(LANES)
    for copy in sends:
        copy.wait_send()


def drain(tg_ref, wg_ref, gg_ref, tg_out, wg_out, gg_out, sem):
    copies = [
        pltpu.make_async_copy(src, dst, sem.at[n])
        for n, (src, dst) in enumerate(((tg_ref, tg_out), (wg_ref, wg_out), (gg_ref, gg_out)))
    ]
    for copy in copies:
        copy.start()
    for copy in copies:
        copy.wait()


def fused(n_rep, n_grp, tokens, norm_gain, key_weight, key_grad):
    n_tok, features = tokens.shape
    rows, keys = key_weight.shape
    cols, n_z = keys // n_rep, n_grp // 2
    grad_scale = (n_tok * n_rep * n_grp) ** (-0.5)
    vmem = pl.BlockSpec(memory_space=pltpu.VMEM)
    bf16, f32, dma = jnp.bfloat16, jnp.float32, pltpu.SemaphoreType.DMA
    block = (rows, cols)
    token_grad, weight_grad, gain_grad = pl.pallas_call(
        functools.partial(kernel, n_z, grad_scale),
        out_shape=(
            jax.ShapeDtypeStruct((n_tok, features), bf16),
            jax.ShapeDtypeStruct(block, f32),
            jax.ShapeDtypeStruct((features,), f32),
        ),
        in_specs=[pl.BlockSpec(memory_space=pltpu.HBM)] * 4,
        out_specs=(vmem,) * 3,
        scratch_shapes=[
            pltpu.VMEM((n_tok, features), bf16),
            pltpu.VMEM((features,), f32),
            pltpu.VMEM((n_tok, keys), bf16),
            dma((4,)),
            pltpu.VMEM((features, keys), bf16),
            pltpu.VMEM((features, n_tok), bf16),
            pltpu.VMEM((n_tok, features), f32),
            pltpu.VMEM((n_z, 2, 2) + block, bf16),
            pltpu.VMEM((n_z, 2, 2) + block, bf16),
            pltpu.VMEM((n_z, 2, 2) + block, bf16),
            pltpu.VMEM((n_z, 2) + block, bf16),
            pltpu.VMEM((n_z,) + block, bf16),
            pltpu.VMEM((n_z,) + block, bf16),
            pltpu.VMEM((2, 1, features), f32),
            pltpu.VMEM((2 * n_z + 2, 1, features), f32),
            dma((4, 2, n_z, 2)), dma((2, 2, n_z, 2)),
            dma((n_z,)), dma((n_z,)),
            dma((n_z, 2)), dma((n_z, 2)),
            dma((n_z,)), dma((n_z,)),
            dma((n_z,)), dma((n_z,)),
            dma((2 * n_z + 2,)), dma((2 * n_z + 2,)),
        ],
        compiler_params=pltpu.CompilerParams(
            collective_id=0, has_side_effects=True, vmem_limit_bytes=40 * 1024 * 1024
        ),
    )(*(pltpu.with_memory_space_constraint(a, pltpu.MemorySpace.HBM) for a in (tokens, norm_gain, key_weight, key_grad)))
    return pl.pallas_call(
        drain,
        out_shape=tuple(jax.ShapeDtypeStruct(a.shape, a.dtype) for a in (token_grad, weight_grad, gain_grad)),
        in_specs=[vmem] * 3,
        out_specs=(pl.BlockSpec(memory_space=pl.ANY),) * 3,
        scratch_shapes=[dma((3,))],
        compiler_params=pltpu.CompilerParams(vmem_limit_bytes=8 * 1024 * 1024),
    )(token_grad, weight_grad, gain_grad)


def plain(tokens, norm_gain, key_weight, key_grad):
    total_tokens = tokens.shape[0] * lax.axis_size("rep") * lax.axis_size("grp")
    grad_scale = total_tokens ** (-0.5)
    wide_tokens = tokens.astype(jnp.float32)
    inv_rms = lax.rsqrt(jnp.mean(wide_tokens * wide_tokens, axis=1, keepdims=True) + epsilon)
    normed = (wide_tokens * inv_rms * norm_gain).astype(jnp.bfloat16)
    partial_value = lax.dot_general(
        normed, key_grad, (((0,), (0,)), ((), ())), preferred_element_type=jnp.float32
    )
    d_normed = lax.dot_general(
        key_grad,
        lax.all_gather(key_weight, "grp", axis=0, tiled=True),
        (((1,), (1,)), ((), ())),
        preferred_element_type=jnp.float32,
    )
    section_one = lax.psum_scatter(
        partial_value.astype(jnp.bfloat16), "rep", scatter_dimension=1, tiled=True
    ).astype(jnp.float32)
    weight_sum = lax.psum_scatter(section_one, "grp", scatter_dimension=0, tiled=True)
    gain_local = jnp.sum(d_normed * wide_tokens * inv_rms, axis=0)
    gain_total = lax.psum(gain_local, ("rep", "grp"))
    scaled = d_normed * norm_gain
    inner_mean = jnp.mean(scaled * wide_tokens, axis=1, keepdims=True)
    token_grad = (inv_rms * (scaled - wide_tokens * inv_rms * inv_rms * inner_mean)).astype(
        jnp.bfloat16
    )
    return (token_grad, weight_sum * grad_scale, gain_total * grad_scale)


def shards(tokens, norm_gain, key_weight, key_grad):
    n_rep, n_grp = lax.axis_size("rep"), lax.axis_size("grp")
    n_z = n_grp // 2
    if (
        n_rep == 2 * 2 and n_grp == 2 * 4
        and key_weight.shape[1] % (n_rep * LANES) == 0 and key_weight.shape[0] % 16 == 0
        and tokens.shape[1] % (2 * LANES) == 0 and tokens.shape[0] % LANES == 0
    ):
        return fused(n_rep, n_grp, tokens, norm_gain, key_weight, key_grad)
    return plain(tokens, norm_gain, key_weight, key_grad)


def solution(mesh):
    in_specs = (P(("rep", "grp"), None), P(), P("grp", None), P(("rep", "grp"), None))
    out_specs = (P(("rep", "grp"), None), P("grp", "rep"), P())
    return jax.shard_map(shards, mesh=mesh, in_specs=in_specs, out_specs=out_specs, check_vma=False)
```

```python
import functools

import jax
import jax.numpy as jnp
from jax import lax
from jax.experimental import pallas as pl
from jax.experimental.pallas import tpu as pltpu
from jax.sharding import PartitionSpec as P

epsilon = 1e-06
MESH = pl.DeviceIdType.MESH
LANES = 128


def flip(i, bits):
    bit = 1
    while bit <= bits:
        if bits & bit:
            i = i + bit * (1 - 2 * lax.rem(lax.div(i, bit), 2))
        bit *= 2
    return i


HA, HR = 2, 2
PIECE, HOP, LEAD, AHEAD = 3.16, 1.9, 0.8, 10.0
PART_ORDER = [(3, 0), (2, 0), (3, 1), (2, 1), (0, 0), (1, 0), (0, 1), (1, 1)]


def messages():
    out = []

    def add(role, link, what, dst, arrives, needs, size):
        out.append(dict(role=role, link=link, what=what, dst=dst, arrives=arrives, needs=needs, size=size))

    for h in range(HA):
        size = PIECE / HA
        for role, me in (("E", 0), ("I", 1)):
            for q in (0, 1):
                for k in range(4):
                    needs = ("own",) if k == me else ("W", q, k, 0, h)
                    if q == 0:
                        add(role, "y", ("W", q, k, 0, h), role, ("W", q, k, 1, h), [needs], size)
                        add(role, "x", ("W", q, k, 1, h), role, ("W", 1, k, 1, h), [("W", 0, k, 1, h)], size)
                    if role == "E" and k == 0:
                        add(role, "z", ("W", q, k, 0, h), "I", ("W", q, 0, 0, h), [needs], size)
                    if role == "I" and k >= 1:
                        add(role, "z", ("W", q, k, 0, h), "E", ("W", q, k, 0, h), [needs], size)
                    if role == "I" and k <= 1:
                        add(role, "across", ("W", q, k, 0, h), "I", ("W", q, 3 - k, 0, h), [needs], size)
    for h in range(HR):
        size = PIECE / HR
        for s in (0, 1):
            for role in "EI":
                for k in range(4):
                    link = "x" if k in (0, 3) else "y"
                    add(role, link, ("one", k, s, h), role, ("in1", k, s, h), [("part", k, s, 1)], size)
            for k in (1, 2, 3):
                needs = [("part", k, s, 0), ("in1", k, s, h)]
                add("E", "z", ("sum", k, s, h), "I", ("inz", k, s, h), needs, size)
                if k > 1:
                    needs = needs + [("inz", k, s, h)]
                    add("I", "across", ("sum", k, s, h), "I", ("inx", 3 - k, s, h), needs, size)
            needs = [("part", 0, s, 0), ("in1", 0, s, h), ("inx", 0, s, h)]
            add("I", "z", ("sum", 0, s, h), "E", ("inz", 0, s, h), needs, size)
        needs = [("part", 0, 1, 0), ("in1", 0, 1, h), ("inz", 0, 1, h)]
        add("E", "y", ("sum", 0, 1, h), "E", ("fin", h), needs, size)
        needs = [("part", 1, 1, 0), ("in1", 1, 1, h), ("inz", 1, 1, h), ("inx", 1, 1, h)]
        add("I", "x", ("sum", 1, 1, h), "I", ("fin", h), needs, size)
    return out


def plan():
    copies = messages()
    known, users, tails = {}, {}, {}
    for role in "EI":
        known[role, ("own",)] = 0.9
        for i, (k, s) in enumerate(PART_ORDER):
            known[role, ("part", k, s, 1)] = 3.2 + 0.12 * i
            known[role, ("part", k, s, 0)] = 3.2 + 0.12 * (8 + i)
    for i, copy in enumerate(copies):
        for need in copy["needs"]:
            users.setdefault((copy["role"], need), []).append(i)

    def tail(i):
        if i not in tails:
            copy = copies[i]
            rest = AHEAD if copy["arrives"][0] == "W" else 1.5
            for j in users.get((copy["dst"], copy["arrives"]), []):
                rest = max(rest, tail(j))
            tails[i] = rest + copy["size"] + HOP
        return tails[i]

    free, left = {}, list(range(len(copies)))
    while left:
        best = None
        for i in left:
            copy = copies[i]
            needs = [(copy["role"], need) for need in copy["needs"]]
            if all(need in known for need in needs):
                link = free.get((copy["role"], copy["link"]), 0.0)
                ready = max(known[need] for need in needs)
                key = (round(max(link, ready), 3), -tail(i), i)
                if best is None or key < best[0]:
                    best = (key, i, ready)
        (start, _, _), i, ready = best
        copy = copies[i]
        left.remove(i)
        copy["start"], copy["ready"] = start, ready
        free[copy["role"], copy["link"]] = start + copy["size"]
        known[copy["dst"], copy["arrives"]] = start + copy["size"] + HOP
    steps = {}
    for role in "EI":
        todo = [(1.0, 0, ("norm",))]
        for k, s in PART_ORDER:
            for o in (1, 0):
                todo.append((known[role, ("part", k, s, o)], 1, ("part", k, s, o)))
        got = [(t, what) for (r, what), t in known.items() if r == role and what[0] == "W"]
        for t, what in got:
            todo.append((t, 2, what))
        near = max(t for t, what in got if what[2] < 2) + 1.4
        far = max(max(t for t, what in got) + 1.4, near + 1.8)
        for j in range(3):
            todo.append((near + 0.55 * j, 3, ("dot", 0, j)))
            todo.append((far + 0.55 * j, 3, ("dot", 1, j)))
        todo.append((far + 1.6, 3, ("gain", 1)))
        todo.append((far + 3.8, 3, ("gain", 2)))
        for j in range(3):
            todo.append((far + 1.7 + 0.2 * j, 4, ("grad", j)))
        for i, copy in enumerate(copies):
            if copy["role"] == role:
                todo.append((max(copy["ready"], copy["start"] - LEAD), 5 + i, ("send", copy)))
        steps[role] = [step for _, _, step in sorted(todo, key=lambda a: a[:2])]
    return steps


def kernel(
    n_z, grad_scale,
    tok_hbm, gain_hbm, w_hbm, kg_hbm,
    tg_ref, wg_ref, gg_ref,
    tok_ref, gain_ref, kg_ref, load_sem, wfull, normed, kgq, inv_ref, inner, dn, part, in1, inz, inx, fin, gsend, grecv, gain_row,
    send_sem, w_recv, c_recv, in1_recv, inz_recv, inx_recv, fin_recv, n_recv, k_recv, g_recv,
):
    rep, grp = lax.axis_index("rep"), lax.axis_index("grp")
    x, c = lax.div(rep, 2), lax.rem(rep, 2)
    z, y = lax.div(grp, 2), lax.rem(grp, 2)
    upper = lax.div(z, 2)
    n_tok, features = tok_ref.shape
    rows, cols = fin.shape
    peer_c = (2 * x + 1 - c, grp)
    peer_x = (2 * (1 - x) + c, grp)
    peer_cx = (2 * (1 - x) + 1 - c, grp)
    peer_y = (rep, 2 * z + 1 - y)
    peer_z = [None] + [(rep, 2 * flip(z, k) + y) for k in range(1, n_z)]
    group = [peer_y]
    for k in range(1, n_z):
        group += [peer_z[k], (rep, 2 * flip(z, k) + 1 - y)]
    bf16, f32 = jnp.bfloat16, jnp.float32

    def row_at(k, yy, h=0, parts=1):
        g = 2 * (k + upper * (3 - 2 * k)) + (1 - y if yy else y)
        return pl.ds(pl.multiple_of(g * rows + h * (rows // parts), 16), rows // parts)

    def col_at(xx):
        r = 2 * (1 - x if xx else x) + c
        return pl.ds(pl.multiple_of(r * cols, LANES), cols)

    own_rows = pl.ds(pl.multiple_of(grp * rows, 16), rows)
    loads = [
        pltpu.make_async_copy(src, dst, load_sem.at[n])
        for n, (src, dst) in enumerate(
            ((w_hbm, wfull.at[own_rows, :]), (tok_hbm, tok_ref), (kg_hbm, kg_ref), (gain_hbm, gain_ref))
        )
    ]
    for load in loads:
        load.start()

    barrier = pltpu.get_barrier_semaphore()
    peers = [peer_c, peer_x, peer_cx] + group
    for peer in peers:
        pl.semaphore_signal(barrier, inc=1, device_id=peer, device_id_type=MESH)
    pl.semaphore_wait(barrier, len(peers))
    loads[0].wait()

    def role(name, steps):
        sends = []

        def send(src, dst, r_sem, peer):
            copy = pltpu.make_async_remote_copy(
                src_ref=src, dst_ref=dst, send_sem=send_sem.at[len(sends)], recv_sem=r_sem,
                device_id=peer, device_id_type=MESH,
            )
            copy.start()
            sends.append(copy)

        waited = set()

        def arrived(dst, sem, key):
            if key not in waited:
                waited.add(key)
                pltpu.make_async_remote_copy(
                    src_ref=dst, dst_ref=dst, send_sem=sem, recv_sem=sem, device_id=peer_c, device_id_type=MESH
                ).wait_recv()

        def split(h):
            return pl.ds(h * (rows // HR), rows // HR)

        def w_piece(q, k, yy, h):
            return wfull.at[row_at(k, yy, h, HA), col_at(q)]

        def got(what):
            kind = what[0]
            if kind == "W":
                _, q, k, yy, h = what
                arrived(w_piece(q, k, yy, h), w_recv.at[q, k, yy, h], what)
            elif kind == "fin":
                arrived(fin.at[split(what[1]), :], fin_recv.at[what[1]], what)
            elif kind in ("in1", "inz", "inx"):
                _, k, s, h = what
                buf, sem = {"in1": (in1, in1_recv), "inz": (inz, inz_recv), "inx": (inx, inx_recv)}[kind]
                arrived(buf.at[k, s, split(h), :], sem.at[k, s, h], what)

        def summed(k, s, h):
            at = split(h)
            total = part[k, s, 0, at, :].astype(f32)
            terms = [("in1", in1)]
            if name == "E":
                terms += [("inz", inz)] if k == 0 else []
            else:
                terms += ([("inz", inz)] if k > 0 else []) + ([("inx", inx)] if k < 2 else [])
            for kind, buf in terms:
                got((kind, k, s, h))
                total = total + buf[k, s, at, :].astype(f32)
            return total

        def send_copy(copy):
            what, arrives, link = copy["what"], copy["arrives"], copy["link"]
            peer = {"x": peer_x, "y": peer_y, "z": peer_z[1], "across": peer_z[3]}[link]
            for need in copy["needs"]:
                got(need)
            if what[0] == "W":
                _, q, k, yy, h = what
                piece = w_piece(q, k, yy, h)
                send(piece, piece, w_recv.at[arrives[1:]], peer)
                return
            if arrives[0] == "fin":
                dst, sem = fin.at[split(arrives[1]), :], fin_recv.at[arrives[1]]
            else:
                _, k, s, h = arrives
                buf, sems = {"in1": (in1, in1_recv), "inz": (inz, inz_recv), "inx": (inx, inx_recv)}[arrives[0]]
                dst, sem = buf.at[k, s, split(h), :], sems.at[k, s, h]
            _, k, s, h = what
            if what[0] == "one":
                send(part.at[k, s, 1, split(h), :], dst, sem, peer)
            else:
                part[k, s, 0, split(h), :] = summed(k, s, h).astype(bf16)
                send(part.at[k, s, 0, split(h), :], dst, sem, peer)

        def norm():
            loads[1].wait()
            acc = None
            for j in range(features // LANES):
                t = tok_ref[:, j * LANES:(j + 1) * LANES].astype(f32)
                acc = t * t if acc is None else acc + t * t
            inv = lax.rsqrt(jnp.sum(acc, axis=1, keepdims=True) / features + epsilon)
            inv_ref[...] = inv
            inner[...] = jnp.zeros_like(inner)
            loads[3].wait()
            for j in range(features // LANES):
                at = slice(j * LANES, (j + 1) * LANES)
                t = tok_ref[:, at].astype(f32)
                normed[at, :n_tok] = (t * inv * gain_ref[at].reshape(1, -1)).T.astype(bf16)
            loads[2].wait()
            for xx in (0, 1):
                kgq[xx, :n_tok, :] = kg_ref[:, col_at(xx)]
                theirs = pl.ds(pl.multiple_of((2 * (1 - x if xx else x) + 1 - c) * cols, LANES), cols)
                send(kg_ref.at[:, theirs], kgq.at[xx, pl.ds(n_tok, n_tok), :], k_recv.at[xx], peer_c)
            for k, yy in ((3, 0), (2, 1), (3, 1), (0, 0), (1, 1), (0, 1), (2, 0), (1, 0)):
                send(
                    normed.at[row_at(k, yy), pl.ds(0, n_tok)], normed.at[row_at(k, yy), pl.ds(n_tok, n_tok)],
                    n_recv.at[k, yy], peer_c,
                )

        def block(k, s, o):
            yy, xx = (s, o) if k in (0, 3) else (o, s)
            arrived(kgq.at[xx, pl.ds(n_tok, n_tok), :], k_recv.at[xx], ("kg", xx))
            arrived(normed.at[row_at(k, yy), pl.ds(n_tok, n_tok)], n_recv.at[k, yy], ("normed", k, yy))
            part[k, s, o] = jnp.dot(
                normed[row_at(k, yy), :], kgq[xx], preferred_element_type=f32
            ).astype(bf16)

        me = 0 if name == "E" else 1

        def dots(far, j):
            if j == 0:
                for k in (2, 3) if far else (0, 1):
                    for yy in (0, 1):
                        if (k, yy) != (me, 0):
                            for q in (0, 1):
                                for h in range(HA):
                                    got(("W", q, k, yy, h))
                                    at = (row_at(k, yy, h, HA), other_col(q))
                                    arrived(wfull.at[at], c_recv.at[q, k, yy, h], ("C", q, k, yy, h))
            wide = features // 6
            base = (1 - upper if far else upper) * (features // 2) + j * wide
            at = pl.ds(pl.multiple_of(base, LANES), wide)
            d = lax.dot_general(
                kg_ref[...], wfull[at, :], (((1,), (1,)), ((), ())), preferred_element_type=f32
            )
            dn[:, at] = d
            dt = d * tok_ref[:, at].astype(f32)
            gsend[0, :, at] = jnp.sum(dt * inv_ref[...], axis=0, keepdims=True)
            gain_at = gain_row[:, at]
            scaled = dt * gain_at
            add = scaled[:, :LANES]
            for n in range(1, wide // LANES):
                add = add + scaled[:, n * LANES:(n + 1) * LANES]
            inner[...] = inner[...] + add

        def other_col(q):
            r = 2 * (1 - x if q else x) + 1 - c
            return pl.ds(pl.multiple_of(r * cols, LANES), cols)

        def gain(stage):
            if stage == 1:
                for n, peer in enumerate((peer_c, peer_x, peer_cx)):
                    send(gsend.at[0], grecv.at[n], g_recv.at[n], peer)
                return
            for n in range(3):
                arrived(grecv.at[n], g_recv.at[n], ("g", n))
            gsend[1] = (gsend[0] + grecv[0]) + (grecv[1] + grecv[2])
            for n, peer in enumerate(group):
                send(gsend.at[1], grecv.at[3 + n], g_recv.at[3 + n], peer)

        def grad(j):
            inv = inv_ref[...]
            pull = inv * inv * (jnp.sum(inner[...], axis=1, keepdims=True) / features)
            wide = features // 9
            for n in range(3 * j, 3 * j + 3):
                at = slice(n * wide, (n + 1) * wide)
                t = tok_ref[:, at].astype(f32)
                tg_ref[:, at] = (inv * (dn[:, at] * gain_ref[at].reshape(1, -1) - t * pull)).astype(bf16)

        for step in steps:
            kind = step[0]
            if kind == "send":
                send_copy(step[1])
            elif kind == "norm":
                norm()
                for j in range(features // LANES):
                    at = slice(j * LANES, (j + 1) * LANES)
                    gain_row[:, at] = gain_ref[at].reshape(1, -1)
            elif kind == "part":
                block(*step[1:])
            elif kind == "W":
                _, q, k, yy, h = step
                got(step)
                piece = w_piece(q, k, yy, h)
                send(piece, piece, c_recv.at[q, k, yy, h], peer_c)
            elif kind == "dot":
                dots(*step[1:])
            elif kind == "gain":
                gain(step[1])
            else:
                grad(step[1])

        for h in range(HR):
            total = summed(me, 0, h)
            got(("fin", h))
            wg_ref[split(h), :] = (total + fin[split(h), :].astype(f32)) * grad_scale
        terms = [gsend[1]]
        for n in range(3, 3 + len(group)):
            arrived(grecv.at[n], g_recv.at[n], ("g", n))
            terms.append(grecv[n])
        while len(terms) > 1:
            terms = [terms[i] + terms[i + 1] for i in range(0, len(terms), 2)]
        total = terms[0] * grad_scale
        for j in range(features // LANES):
            at = slice(j * LANES, (j + 1) * LANES)
            gg_ref[at] = total[:, at].reshape(LANES)
        for copy in sends:
            copy.wait_send()

    steps = plan()
    end = lax.rem(lax.div(z + 1, 2), 2) == 0
    for name, here in (("E", end), ("I", jnp.logical_not(end))):
        pl.when(here)(functools.partial(role, name, steps[name]))


def drain(tg_ref, wg_ref, gg_ref, tg_out, wg_out, gg_out, sem):
    copies = [
        pltpu.make_async_copy(src, dst, sem.at[n])
        for n, (src, dst) in enumerate(((tg_ref, tg_out), (wg_ref, wg_out), (gg_ref, gg_out)))
    ]
    for copy in copies:
        copy.start()
    for copy in copies:
        copy.wait()


def fused(n_rep, n_grp, tokens, norm_gain, key_weight, key_grad):
    n_tok, features = tokens.shape
    rows, keys = key_weight.shape
    cols, n_z = keys // n_rep, n_grp // 2
    grad_scale = (n_tok * n_rep * n_grp) ** (-0.5)
    vmem = pl.BlockSpec(memory_space=pltpu.VMEM)
    bf16, f32, dma = jnp.bfloat16, jnp.float32, pltpu.SemaphoreType.DMA
    block = (rows, cols)
    token_grad, weight_grad, gain_grad = pl.pallas_call(
        functools.partial(kernel, n_z, grad_scale),
        out_shape=(
            jax.ShapeDtypeStruct((n_tok, features), bf16),
            jax.ShapeDtypeStruct(block, f32),
            jax.ShapeDtypeStruct((features,), f32),
        ),
        in_specs=[pl.BlockSpec(memory_space=pltpu.HBM)] * 4,
        out_specs=(vmem,) * 3,
        scratch_shapes=[
            pltpu.VMEM((n_tok, features), bf16),
            pltpu.VMEM((features,), f32),
            pltpu.VMEM((n_tok, keys), bf16),
            dma((4,)),
            pltpu.VMEM((features, keys), bf16),
            pltpu.VMEM((features, 2 * n_tok), bf16),
            pltpu.VMEM((2, 2 * n_tok, cols), bf16),
            pltpu.VMEM((n_tok, 1), f32),
            pltpu.VMEM((n_tok, LANES), f32),
            pltpu.VMEM((n_tok, features), f32),
            pltpu.VMEM((n_z, 2, 2) + block, bf16),
            pltpu.VMEM((n_z, 2) + block, bf16),
            pltpu.VMEM((n_z, 2) + block, bf16),
            pltpu.VMEM((2, 2) + block, bf16),
            pltpu.VMEM(block, bf16),
            pltpu.VMEM((2, 1, features), f32),
            pltpu.VMEM((2 * n_z + 2, 1, features), f32),
            pltpu.VMEM((1, features), f32),
            dma((160,)),
            dma((2, n_z, 2, HA)), dma((2, n_z, 2, HA)),
            dma((n_z, 2, HR)), dma((n_z, 2, HR)), dma((2, 2, HR)), dma((HR,)),
            dma((n_z, 2)), dma((2,)), dma((2 * n_z + 2,)),
        ],
        compiler_params=pltpu.CompilerParams(
            collective_id=0, has_side_effects=True, vmem_limit_bytes=40 * 1024 * 1024
        ),
    )(*(pltpu.with_memory_space_constraint(a, pltpu.MemorySpace.HBM) for a in (tokens, norm_gain, key_weight, key_grad)))
    return pl.pallas_call(
        drain,
        out_shape=tuple(jax.ShapeDtypeStruct(a.shape, a.dtype) for a in (token_grad, weight_grad, gain_grad)),
        in_specs=[vmem] * 3,
        out_specs=(pl.BlockSpec(memory_space=pl.ANY),) * 3,
        scratch_shapes=[dma((3,))],
        compiler_params=pltpu.CompilerParams(vmem_limit_bytes=8 * 1024 * 1024),
    )(token_grad, weight_grad, gain_grad)


def plain(tokens, norm_gain, key_weight, key_grad):
    total_tokens = tokens.shape[0] * lax.axis_size("rep") * lax.axis_size("grp")
    grad_scale = total_tokens ** (-0.5)
    wide_tokens = tokens.astype(jnp.float32)
    inv_rms = lax.rsqrt(jnp.mean(wide_tokens * wide_tokens, axis=1, keepdims=True) + epsilon)
    normed = (wide_tokens * inv_rms * norm_gain).astype(jnp.bfloat16)
    partial_value = lax.dot_general(
        normed, key_grad, (((0,), (0,)), ((), ())), preferred_element_type=jnp.float32
    )
    d_normed = lax.dot_general(
        key_grad,
        lax.all_gather(key_weight, "grp", axis=0, tiled=True),
        (((1,), (1,)), ((), ())),
        preferred_element_type=jnp.float32,
    )
    section_one = lax.psum_scatter(
        partial_value.astype(jnp.bfloat16), "rep", scatter_dimension=1, tiled=True
    ).astype(jnp.float32)
    weight_sum = lax.psum_scatter(section_one, "grp", scatter_dimension=0, tiled=True)
    gain_local = jnp.sum(d_normed * wide_tokens * inv_rms, axis=0)
    gain_total = lax.psum(gain_local, ("rep", "grp"))
    scaled = d_normed * norm_gain
    inner_mean = jnp.mean(scaled * wide_tokens, axis=1, keepdims=True)
    token_grad = (inv_rms * (scaled - wide_tokens * inv_rms * inv_rms * inner_mean)).astype(
        jnp.bfloat16
    )
    return (token_grad, weight_sum * grad_scale, gain_total * grad_scale)


def shards(tokens, norm_gain, key_weight, key_grad):
    n_rep, n_grp = lax.axis_size("rep"), lax.axis_size("grp")
    n_z = n_grp // 2
    if (
        n_rep == 2 * 2 and n_grp == 2 * 4
        and key_weight.shape[1] % (n_rep * LANES) == 0 and key_weight.shape[0] % 32 == 0
        and tokens.shape[1] % (18 * LANES) == 0 and tokens.shape[0] % LANES == 0
    ):
        return fused(n_rep, n_grp, tokens, norm_gain, key_weight, key_grad)
    return plain(tokens, norm_gain, key_weight, key_grad)


def solution(mesh):
    in_specs = (P(("rep", "grp"), None), P(), P("grp", None), P(("rep", "grp"), None))
    out_specs = (P(("rep", "grp"), None), P("grp", "rep"), P())
    return jax.shard_map(shards, mesh=mesh, in_specs=in_specs, out_specs=out_specs, check_vma=False)
```

```python
import functools

import jax
import jax.numpy as jnp
from jax import lax
from jax.experimental import pallas as pl
from jax.experimental.pallas import tpu as pltpu
from jax.sharding import PartitionSpec as P

epsilon = 1e-06
MESH = pl.DeviceIdType.MESH
LANES = 128


def flip(i, bits):
    bit = 1
    while bit <= bits:
        if bits & bit:
            i = i + bit * (1 - 2 * lax.rem(lax.div(i, bit), 2))
        bit *= 2
    return i


HA, HR = 2, 3
PIECE, HOP, LEAD, AHEAD = 3.2, 2.5, 1.2, 11.0
OWN, PART, STEP, GUARD = 0.4, 2.7, 0.45, 1.0
XF = {(0, 0), (1, 0), (1, 1), (2, 0), (2, 1), (3, 0)}
PART_ORDER = [(3, 1), (2, 1), (2, 0), (3, 0), (0, 1), (1, 1), (1, 0), (0, 0)]


def messages():
    out = []

    def add(role, link, what, dst, arrives, needs, size):
        out.append(dict(role=role, link=link, what=what, dst=dst, arrives=arrives, needs=needs, size=size))

    for h in range(HA):
        size = PIECE / HA
        for role, me in (("E", 0), ("I", 1)):
            for q in (0, 1):
                for k in range(4):
                    needs = ("own",) if k == me else ("W", q, k, 0, h)
                    if q == 0:
                        add(role, "y", ("W", q, k, 0, h), role, ("W", q, k, 1, h), [needs], size)
                        add(role, "x", ("W", q, k, 1, h), role, ("W", 1, k, 1, h), [("W", 0, k, 1, h)], size)
                    if role == "E" and k == 0:
                        add(role, "z", ("W", q, k, 0, h), "I", ("W", q, 0, 0, h), [needs], size)
                    if role == "I" and k >= 1:
                        add(role, "z", ("W", q, k, 0, h), "E", ("W", q, k, 0, h), [needs], size)
                    if role == "I" and k <= 1:
                        add(role, "across", ("W", q, k, 0, h), "I", ("W", q, 3 - k, 0, h), [needs], size)
    for h in range(HR):
        size = PIECE / HR
        for s in (0, 1):
            for role in "EI":
                for k in range(4):
                    first = (k, h) in XF
                    link, needs = ("x", ("part", k, 1)) if first else ("y", ("part", k, s))
                    add(role, link, ("one", k, s, h), role, ("in1", k, s, h), [needs], size)
            kept = [("part", k, 0 if (k, h) in XF else s) for k in range(4)]
            for k in (1, 2, 3):
                needs = [kept[k], ("in1", k, s, h)]
                add("E", "z", ("sum", k, s, h), "I", ("inz", k, s, h), needs, size)
                if k > 1:
                    needs = needs + [("inz", k, s, h)]
                    add("I", "across", ("sum", k, s, h), "I", ("inx", 3 - k, s, h), needs, size)
            needs = [kept[0], ("in1", 0, s, h), ("inx", 0, s, h)]
            add("I", "z", ("sum", 0, s, h), "E", ("inz", 0, s, h), needs, size)
        for role, k in (("E", 0), ("I", 1)):
            needs = [kept[k], ("in1", k, 1, h), ("inz", k, 1, h)] + ([("inx", 1, 1, h)] if k else [])
            add(role, "y" if (k, h) in XF else "x", ("sum", k, 1, h), role, ("fin", h), needs, size)
    return out


def plan():
    copies = messages()
    known, users, tails = {}, {}, {}
    for role in "EI":
        known[role, ("own",)] = OWN
        for i, (k, xx) in enumerate(PART_ORDER):
            known[role, ("part", k, xx)] = PART + STEP * i
    for i, copy in enumerate(copies):
        for need in copy["needs"]:
            users.setdefault((copy["role"], need), []).append(i)

    def tail(i):
        if i not in tails:
            copy = copies[i]
            rest = AHEAD if copy["arrives"][0] == "W" else 1.5
            for j in users.get((copy["dst"], copy["arrives"]), []):
                rest = max(rest, tail(j))
            tails[i] = rest + copy["size"] + HOP
        return tails[i]

    def schedule(known, blocked):
        free, left = {}, list(range(len(copies)))
        while left:
            best = None
            for i in left:
                copy = copies[i]
                needs = [(copy["role"], need) for need in copy["needs"]]
                if all(need in known for need in needs):
                    ready = max(known[need] for need in needs)
                    start = max(free.get((copy["role"], copy["link"]), 0.0), ready)
                    low, high = blocked.get((copy["role"], copy["link"]), (0.0, 0.0))
                    start = high if low < start < high else start
                    key = (round(start, 3), -tail(i), i)
                    if best is None or key < best[0]:
                        best = (key, i, ready)
            (start, _, _), i, ready = best
            copy = copies[i]
            left.remove(i)
            copy["start"], copy["ready"] = start, ready
            free[copy["role"], copy["link"]] = start + copy["size"]
            known[copy["dst"], copy["arrives"]] = start + copy["size"] + HOP
        return known

    def marks(known, role):
        got = [(t, what) for (r, what), t in known.items() if r == role and what[0] == "W"]
        near = max(t for t, what in got if what[2] < 2) + 2.0
        early = max(max(t for t, what in got if what[2] == 2) + 1.8, near + 1.5)
        far = max(max(t for t, what in got) + 1.4, early + 0.5)
        return got, near, early, far

    first = schedule(dict(known), {})
    blocked = {}
    for role in "EI":
        gain = marks(first, role)[3] + 1.1
        blocked[role, "x"] = (gain - GUARD, gain + 0.1)
    known = schedule(known, blocked)
    steps = {}
    for role in "EI":
        todo = [(0.3, 0, ("norm",))]
        for k, xx in PART_ORDER:
            todo.append((known[role, ("part", k, xx)], 1, ("part", k, xx)))
        got, near, early, far = marks(known, role)
        for t, what in got:
            todo.append((t, 2, what))
        for j in range(3):
            todo.append((near + 0.55 * j, 3, ("dot", 0, j)))
            todo.append((far + 0.55 * (j - 1) if j else early, 3, ("dot", 1, j)))
        gain = marks(first, role)[3] + 1.1
        todo.append((gain, 3, ("gain", 1)))
        last = max(copy["start"] for copy in copies if copy["role"] == role)
        todo.append((max(far + 4.0, last - LEAD + 0.1), 3, ("gain", 2)))
        for j in range(3):
            todo.append((far + 1.7 + 0.2 * j, 4, ("grad", j)))
        for i, copy in enumerate(copies):
            if copy["role"] == role:
                t = copy["start"] - LEAD
                if copy["link"] == "x" and copy["start"] > gain:
                    t = max(t, gain + 0.01)
                t = 0.0 if copy["needs"] == [("own",)] and t < 1.0 else t
                todo.append((max(copy["ready"], t), 5 + i, ("send", copy)))
        steps[role] = [step for _, _, step in sorted(todo, key=lambda a: a[:2])]
    return steps


def kernel(
    n_z, grad_scale,
    tok_hbm, gain_hbm, w_hbm, kg_hbm,
    tg_ref, wg_ref, gg_ref,
    tok_ref, gain_ref, kg_ref, load_sem, wfull, normed, kgq, inv_ref, inner, dn, part, in1, inz, inx, fin, gsend, grecv, gain_row,
    send_sem, w_recv, c_recv, in1_recv, inz_recv, inx_recv, fin_recv, n_recv, k_recv, g_recv,
):
    rep, grp = lax.axis_index("rep"), lax.axis_index("grp")
    x, c = lax.div(rep, 2), lax.rem(rep, 2)
    z, y = lax.div(grp, 2), lax.rem(grp, 2)
    upper = lax.div(z, 2)
    n_tok, features = tok_ref.shape
    rows, cols = fin.shape
    peer_c = (2 * x + 1 - c, grp)
    peer_x = (2 * (1 - x) + c, grp)
    peer_cx = (2 * (1 - x) + 1 - c, grp)
    peer_y = (rep, 2 * z + 1 - y)
    peer_z = [None] + [(rep, 2 * flip(z, k) + y) for k in range(1, n_z)]
    group = [peer_y]
    for k in range(1, n_z):
        group += [peer_z[k], (rep, 2 * flip(z, k) + 1 - y)]
    bf16, f32 = jnp.bfloat16, jnp.float32

    def row_at(k, yy, h=0, parts=1):
        g = 2 * (k + upper * (3 - 2 * k)) + (1 - y if yy else y)
        return pl.ds(pl.multiple_of(g * rows + h * (rows // parts), 16), rows // parts)

    def col_at(xx):
        r = 2 * (1 - x if xx else x) + c
        return pl.ds(pl.multiple_of(r * cols, LANES), cols)

    own_rows = pl.ds(pl.multiple_of(grp * rows, 16), rows)
    loads = [
        pltpu.make_async_copy(src, dst, load_sem.at[n])
        for n, (src, dst) in enumerate(
            ((w_hbm, wfull.at[own_rows, :]), (tok_hbm, tok_ref), (kg_hbm, kg_ref), (gain_hbm, gain_ref))
        )
    ]
    for load in loads:
        load.start()

    end = lax.rem(lax.div(z + 1, 2), 2) == 0
    inside = jnp.logical_not(end)
    barrier = pltpu.get_barrier_semaphore()
    peers = [peer_c, peer_x, peer_y, peer_z[1]]
    for peer in peers:
        pl.semaphore_signal(barrier, inc=1, device_id=peer, device_id_type=MESH)

    @pl.when(inside)
    def _():
        pl.semaphore_signal(barrier, inc=1, device_id=peer_z[3], device_id_type=MESH)

    pl.semaphore_wait(barrier, len(peers) + inside.astype(jnp.int32))
    loads[0].wait()

    def role(name, steps):
        sends = []

        def send(src, dst, r_sem, peer):
            copy = pltpu.make_async_remote_copy(
                src_ref=src, dst_ref=dst, send_sem=send_sem, recv_sem=r_sem,
                device_id=peer, device_id_type=MESH,
            )
            copy.start()
            sends.append(copy)

        waited = set()

        def arrived(dst, sem, key):
            if key not in waited:
                waited.add(key)
                pltpu.make_async_remote_copy(
                    src_ref=dst, dst_ref=dst, send_sem=sem, recv_sem=sem, device_id=peer_c, device_id_type=MESH
                ).wait_recv()

        def split(h):
            return pl.ds(h * (rows // HR), rows // HR)

        def w_piece(q, k, yy, h):
            return wfull.at[row_at(k, yy, h, HA), col_at(q)]

        def got(what):
            kind = what[0]
            if kind == "W":
                _, q, k, yy, h = what
                arrived(w_piece(q, k, yy, h), w_recv.at[q, k, yy, h], what)
            elif kind == "fin":
                arrived(fin.at[split(what[1]), :], fin_recv.at[what[1]], what)
            elif kind in ("in1", "inz", "inx"):
                _, k, s, h = what
                buf, sem = {"in1": (in1, in1_recv), "inz": (inz, inz_recv), "inx": (inx, inx_recv)}[kind]
                k = k - 1 if kind == "inz" and k else k
                arrived(buf.at[k, s, split(h), :], sem.at[k, s, h], what)

        def kept(k, s, h):
            return (k, s, 0, split(h), slice(None)) if (k, h) in XF else (k, 0, s, split(h), slice(None))

        def given(k, s, h):
            return (k, s, 1, split(h), slice(None)) if (k, h) in XF else (k, 1, s, split(h), slice(None))

        def summed(k, s, h):
            at = split(h)
            total = part[kept(k, s, h)].astype(f32)
            terms = [("in1", in1)]
            if name == "E":
                terms += [("inz", inz)] if k == 0 else []
            else:
                terms += ([("inz", inz)] if k > 0 else []) + ([("inx", inx)] if k < 2 else [])
            for kind, buf in terms:
                got((kind, k, s, h))
                slot = k - 1 if kind == "inz" and k else k
                total = total + buf[slot, s, at, :].astype(f32)
            return total

        def send_copy(copy):
            what, arrives, link = copy["what"], copy["arrives"], copy["link"]
            peer = {"x": peer_x, "y": peer_y, "z": peer_z[1], "across": peer_z[3]}[link]
            for need in copy["needs"]:
                got(need)
            if what[0] == "W":
                _, q, k, yy, h = what
                piece = w_piece(q, k, yy, h)
                send(piece, piece, w_recv.at[arrives[1:]], peer)
                return
            if arrives[0] == "fin":
                dst, sem = fin.at[split(arrives[1]), :], fin_recv.at[arrives[1]]
            else:
                _, k, s, h = arrives
                buf, sems = {"in1": (in1, in1_recv), "inz": (inz, inz_recv), "inx": (inx, inx_recv)}[arrives[0]]
                k = k - 1 if arrives[0] == "inz" and k else k
                dst, sem = buf.at[k, s, split(h), :], sems.at[k, s, h]
            _, k, s, h = what
            if what[0] == "one":
                send(part.at[given(k, s, h)], dst, sem, peer)
            else:
                part[kept(k, s, h)] = summed(k, s, h).astype(bf16)
                send(part.at[kept(k, s, h)], dst, sem, peer)

        def norm():
            loads[2].wait()
            for xx in (1, 0):
                theirs = pl.ds(pl.multiple_of((2 * (1 - x if xx else x) + 1 - c) * cols, LANES), cols)
                send(kg_ref.at[:, theirs], kgq.at[xx, pl.ds(n_tok, n_tok), :], k_recv, peer_c)
            loads[1].wait()
            acc = None
            for j in range(features // LANES):
                t = tok_ref[:, j * LANES:(j + 1) * LANES].astype(f32)
                acc = t * t if acc is None else acc + t * t
            inv = lax.rsqrt(jnp.sum(acc, axis=1, keepdims=True) / features + epsilon)
            inv_ref[...] = inv
            inner[...] = jnp.zeros_like(inner)
            loads[3].wait()
            for j in range(features // LANES):
                at = slice(j * LANES, (j + 1) * LANES)
                gain_row[:, at] = gain_ref[at].reshape(1, -1)
            half = features // 2
            for far in (1, 0):
                for j in range(half // LANES):
                    base = (1 - upper if far else upper) * half + j * LANES
                    at = pl.ds(pl.multiple_of(base, LANES), LANES)
                    t = tok_ref[:, at].astype(f32)
                    normed[at, :n_tok] = (t * inv * gain_row[:, at]).T.astype(bf16)
                for k in (3, 2) if far else (0, 1):
                    send(normed.at[pair_at(k), pl.ds(0, n_tok)], theirs_at(k), n_recv.at[k], peer_c)
            for xx in (0, 1):
                kgq[xx, :n_tok, :] = kg_ref[:, col_at(xx)]

        def pair_at(k):
            return pl.ds(pl.multiple_of(2 * rows * (k + upper * (3 - 2 * k)), 16), 2 * rows)

        def theirs_at(k):
            return normed.at[pair_at(k), pl.ds(n_tok, n_tok)]

        def block(k, xx):
            arrived(kgq.at[:, pl.ds(n_tok, n_tok), :], k_recv, "kg")
            arrived(theirs_at(k), n_recv.at[k], ("normed", k))
            both = jnp.dot(normed[pair_at(k), :], kgq[xx], preferred_element_type=f32).astype(bf16)
            part[k, y, xx] = both[:rows]
            part[k, 1 - y, xx] = both[rows:]

        me = 0 if name == "E" else 1

        def dots(far, j):
            for k in ([0, 1] if j == 0 else []) if not far else [2 if j == 0 else 3]:
                shards = [yy for yy in (0, 1) if (k, yy) != (me, 0)]
                for yy in shards:
                    for q in (0, 1):
                        for h in range(HA):
                            got(("W", q, k, yy, h))
                amount = wfull.at[pl.ds(0, len(shards) * rows), pl.ds(0, 2 * cols)]
                arrived(amount, c_recv.at[k], ("C", k))
            wide = features // 6
            side = 1 - upper if far else upper
            base = side * (features // 2) + (j + upper * (2 - 2 * j)) * wide
            at = pl.ds(pl.multiple_of(base, LANES), wide)
            d = lax.dot_general(
                kg_ref[...], wfull[at, :], (((1,), (1,)), ((), ())), preferred_element_type=f32
            )
            dn[:, at] = d
            dt = d * tok_ref[:, at].astype(f32)
            gsend[0, :, at] = jnp.sum(dt * inv_ref[...], axis=0, keepdims=True)
            gain_at = gain_row[:, at]
            scaled = dt * gain_at
            add = scaled[:, :LANES]
            for n in range(1, wide // LANES):
                add = add + scaled[:, n * LANES:(n + 1) * LANES]
            inner[...] = inner[...] + add

        def gain(stage):
            if stage == 1:
                for n, peer in enumerate((peer_c, peer_x, peer_cx)):
                    send(gsend.at[0], grecv.at[n], g_recv.at[0], peer)
                return
            arrived(grecv.at[pl.ds(0, 3)], g_recv.at[0], "g0")
            gsend[1] = (gsend[0] + grecv[0]) + (grecv[1] + grecv[2])
            for n, peer in enumerate(group):
                send(gsend.at[1], grecv.at[3 + n], g_recv.at[1], peer)

        def grad(j):
            inv = inv_ref[...]
            pull = inv * inv * (jnp.sum(inner[...], axis=1, keepdims=True) / features)
            wide = features // 9
            for n in range(3 * j, 3 * j + 3):
                at = slice(n * wide, (n + 1) * wide)
                t = tok_ref[:, at].astype(f32)
                tg_ref[:, at] = (inv * (dn[:, at] * gain_ref[at].reshape(1, -1) - t * pull)).astype(bf16)

        for step in steps:
            kind = step[0]
            if kind == "send":
                send_copy(step[1])
            elif kind == "norm":
                norm()
            elif kind == "part":
                block(*step[1:])
            elif kind == "W":
                _, q, k, yy, h = step
                got(step)
                piece = w_piece(q, k, yy, h)
                send(piece, piece, c_recv.at[k], peer_c)
            elif kind == "dot":
                dots(*step[1:])
            elif kind == "gain":
                gain(step[1])
            else:
                grad(step[1])

        for h in range(HR):
            total = summed(me, 0, h)
            got(("fin", h))
            wg_ref[split(h), :] = (total + fin[split(h), :].astype(f32)) * grad_scale
        terms = [gsend[1]]
        arrived(grecv.at[pl.ds(3, len(group))], g_recv.at[1], "g1")
        for n in range(3, 3 + len(group)):
            terms.append(grecv[n])
        while len(terms) > 1:
            terms = [terms[i] + terms[i + 1] for i in range(0, len(terms), 2)]
        total = terms[0] * grad_scale
        for j in range(features // LANES):
            at = slice(j * LANES, (j + 1) * LANES)
            gg_ref[at] = total[:, at].reshape(LANES)
        for copy in sends:
            copy.wait_send()

    steps = plan()
    for name, here in (("E", end), ("I", inside)):
        pl.when(here)(functools.partial(role, name, steps[name]))


def drain(tg_ref, wg_ref, gg_ref, tg_out, wg_out, gg_out, sem):
    copies = [
        pltpu.make_async_copy(src, dst, sem.at[n])
        for n, (src, dst) in enumerate(((tg_ref, tg_out), (wg_ref, wg_out), (gg_ref, gg_out)))
    ]
    for copy in copies:
        copy.start()
    for copy in copies:
        copy.wait()


def fused(n_rep, n_grp, tokens, norm_gain, key_weight, key_grad):
    n_tok, features = tokens.shape
    rows, keys = key_weight.shape
    cols, n_z = keys // n_rep, n_grp // 2
    grad_scale = (n_tok * n_rep * n_grp) ** (-0.5)
    vmem = pl.BlockSpec(memory_space=pltpu.VMEM)
    bf16, f32, dma = jnp.bfloat16, jnp.float32, pltpu.SemaphoreType.DMA
    block = (rows, cols)
    token_grad, weight_grad, gain_grad = pl.pallas_call(
        functools.partial(kernel, n_z, grad_scale),
        out_shape=(
            jax.ShapeDtypeStruct((n_tok, features), bf16),
            jax.ShapeDtypeStruct(block, f32),
            jax.ShapeDtypeStruct((features,), f32),
        ),
        in_specs=[pl.BlockSpec(memory_space=pltpu.HBM)] * 4,
        out_specs=(vmem,) * 3,
        scratch_shapes=[
            pltpu.VMEM((n_tok, features), bf16),
            pltpu.VMEM((features,), f32),
            pltpu.VMEM((n_tok, keys), bf16),
            dma((4,)),
            pltpu.VMEM((features, keys), bf16),
            pltpu.VMEM((features, 2 * n_tok), bf16),
            pltpu.VMEM((2, 2 * n_tok, cols), bf16),
            pltpu.VMEM((n_tok, 1), f32),
            pltpu.VMEM((n_tok, LANES), f32),
            pltpu.VMEM((n_tok, features), f32),
            pltpu.VMEM((n_z, 2, 2) + block, bf16),
            pltpu.VMEM((n_z, 2) + block, bf16),
            pltpu.VMEM((n_z - 1, 2) + block, bf16),
            pltpu.VMEM((2, 2) + block, bf16),
            pltpu.VMEM(block, bf16),
            pltpu.VMEM((2, 1, features), f32),
            pltpu.VMEM((2 * n_z + 2, 1, features), f32),
            pltpu.VMEM((1, features), f32),
            dma, dma((2, n_z, 2, HA)), dma((n_z,)),
            dma((n_z, 2, HR)), dma((n_z - 1, 2, HR)), dma((2, 2, HR)), dma((HR,)),
            dma((n_z,)), dma, dma((2,)),
        ],
        compiler_params=pltpu.CompilerParams(
            collective_id=0, has_side_effects=True, vmem_limit_bytes=40 * 1024 * 1024
        ),
    )(*(pltpu.with_memory_space_constraint(a, pltpu.MemorySpace.HBM) for a in (tokens, norm_gain, key_weight, key_grad)))
    return pl.pallas_call(
        drain,
        out_shape=tuple(jax.ShapeDtypeStruct(a.shape, a.dtype) for a in (token_grad, weight_grad, gain_grad)),
        in_specs=[vmem] * 3,
        out_specs=(pl.BlockSpec(memory_space=pl.ANY),) * 3,
        scratch_shapes=[dma((3,))],
        compiler_params=pltpu.CompilerParams(vmem_limit_bytes=8 * 1024 * 1024),
    )(token_grad, weight_grad, gain_grad)


def plain(tokens, norm_gain, key_weight, key_grad):
    total_tokens = tokens.shape[0] * lax.axis_size("rep") * lax.axis_size("grp")
    grad_scale = total_tokens ** (-0.5)
    wide_tokens = tokens.astype(jnp.float32)
    inv_rms = lax.rsqrt(jnp.mean(wide_tokens * wide_tokens, axis=1, keepdims=True) + epsilon)
    normed = (wide_tokens * inv_rms * norm_gain).astype(jnp.bfloat16)
    partial_value = lax.dot_general(
        normed, key_grad, (((0,), (0,)), ((), ())), preferred_element_type=jnp.float32
    )
    d_normed = lax.dot_general(
        key_grad,
        lax.all_gather(key_weight, "grp", axis=0, tiled=True),
        (((1,), (1,)), ((), ())),
        preferred_element_type=jnp.float32,
    )
    section_one = lax.psum_scatter(
        partial_value.astype(jnp.bfloat16), "rep", scatter_dimension=1, tiled=True
    ).astype(jnp.float32)
    weight_sum = lax.psum_scatter(section_one, "grp", scatter_dimension=0, tiled=True)
    gain_local = jnp.sum(d_normed * wide_tokens * inv_rms, axis=0)
    gain_total = lax.psum(gain_local, ("rep", "grp"))
    scaled = d_normed * norm_gain
    inner_mean = jnp.mean(scaled * wide_tokens, axis=1, keepdims=True)
    token_grad = (inv_rms * (scaled - wide_tokens * inv_rms * inv_rms * inner_mean)).astype(
        jnp.bfloat16
    )
    return (token_grad, weight_sum * grad_scale, gain_total * grad_scale)


def shards(tokens, norm_gain, key_weight, key_grad):
    n_rep, n_grp = lax.axis_size("rep"), lax.axis_size("grp")
    n_z = n_grp // 2
    if (
        n_rep == 2 * 2 and n_grp == 2 * 4
        and key_weight.shape[1] % (n_rep * LANES) == 0 and key_weight.shape[0] % 96 == 0
        and tokens.shape[1] % (18 * LANES) == 0 and tokens.shape[0] % LANES == 0
    ):
        return fused(n_rep, n_grp, tokens, norm_gain, key_weight, key_grad)
    return plain(tokens, norm_gain, key_weight, key_grad)


def solution(mesh):
    in_specs = (P(("rep", "grp"), None), P(), P("grp", None), P(("rep", "grp"), None))
    out_specs = (P(("rep", "grp"), None), P("grp", "rep"), P())
    return jax.shard_map(shards, mesh=mesh, in_specs=in_specs, out_specs=out_specs, check_vma=False)
```

```python
import functools

import jax
import jax.numpy as jnp
from jax import lax
from jax.experimental import pallas as pl
from jax.experimental.pallas import tpu as pltpu
from jax.sharding import PartitionSpec as P

epsilon = 1e-06
MESH = pl.DeviceIdType.MESH
LANES = 128


def flip(i, bits):
    bit = 1
    while bit <= bits:
        if bits & bit:
            i = i + bit * (1 - 2 * lax.rem(lax.div(i, bit), 2))
        bit *= 2
    return i


HA, HR = 2, 3
PIECE, HOP, LEAD, AHEAD = 3.2, 2.5, 1.2, 11.0
OWN, PART, STEP, GUARD = 0.4, 2.7, 0.45, 1.0
SECOND, CLEAR = 2.8, 0.8
FAR, AGT, RST = 1.4, 1.0, 1.5
XF = {(0, 0), (0, 1), (1, 0), (1, 1), (2, 0), (2, 1), (3, 0), (3, 1)}
BY_Y = {"E": {(3, 0), (3, 1)}, "I": {(3, 0), (3, 1)}}
PART_ORDER = [(3, 1), (2, 1), (2, 0), (3, 0), (0, 1), (1, 1), (1, 0), (0, 0)]


def messages():
    out = []

    def add(role, link, what, dst, arrives, needs, size):
        out.append(dict(role=role, link=link, what=what, dst=dst, arrives=arrives, needs=needs, size=size))

    for h in range(HA):
        size = PIECE / HA
        for role, me in (("E", 0), ("I", 1)):
            for q in (0, 1):
                for k in range(4):
                    needs = ("own",) if k == me else ("W", q, k, 0, h)
                    if q == 0:
                        add(role, "y", ("W", q, k, 0, h), role, ("W", q, k, 1, h), [needs], size)
                        if (k, h) not in BY_Y[role]:
                            add(role, "x", ("W", q, k, 1, h), role, ("W", 1, k, 1, h), [("W", 0, k, 1, h)], size)
                    elif (k, h) in BY_Y[role]:
                        add(role, "y", ("W", q, k, 0, h), role, ("W", 1, k, 1, h), [needs], size)
                    if role == "E" and k == 0:
                        add(role, "z", ("W", q, k, 0, h), "I", ("W", q, 0, 0, h), [needs], size)
                    if role == "I" and k >= 1:
                        add(role, "z", ("W", q, k, 0, h), "E", ("W", q, k, 0, h), [needs], size)
                    if role == "I" and k <= 1:
                        add(role, "across", ("W", q, k, 0, h), "I", ("W", q, 3 - k, 0, h), [needs], size)
    for h in range(HR):
        size = PIECE / HR
        for s in (0, 1):
            for role in "EI":
                for k in range(4):
                    first = (k, h) in XF
                    link, needs = ("x", ("part", k, 1)) if first else ("y", ("part", k, s))
                    add(role, link, ("one", k, s, h), role, ("in1", k, s, h), [needs], size)
            kept = [("part", k, 0 if (k, h) in XF else s) for k in range(4)]
            for k in (1, 2, 3):
                needs = [kept[k], ("in1", k, s, h)]
                add("E", "z", ("sum", k, s, h), "I", ("inz", k, s, h), needs, size)
                if k > 1:
                    needs = needs + [("inz", k, s, h)]
                    add("I", "across", ("sum", k, s, h), "I", ("inx", 3 - k, s, h), needs, size)
            needs = [kept[0], ("in1", 0, s, h), ("inx", 0, s, h)]
            add("I", "z", ("sum", 0, s, h), "E", ("inz", 0, s, h), needs, size)
        for role, k in (("E", 0), ("I", 1)):
            needs = [kept[k], ("in1", k, 1, h), ("inz", k, 1, h)] + ([("inx", 1, 1, h)] if k else [])
            add(role, "y" if (k, h) in XF else "x", ("sum", k, 1, h), role, ("fin", h), needs, size)
    return out


def plan():
    copies = messages()
    known, users, tails = {}, {}, {}
    for role in "EI":
        known[role, ("own",)] = OWN
        for i, (k, xx) in enumerate(PART_ORDER):
            known[role, ("part", k, xx)] = PART + STEP * i
    for i, copy in enumerate(copies):
        for need in copy["needs"]:
            users.setdefault((copy["role"], need), []).append(i)

    def tail(i):
        if i not in tails:
            copy = copies[i]
            rest = AHEAD if copy["arrives"][0] == "W" else RST
            for j in users.get((copy["dst"], copy["arrives"]), []):
                rest = max(rest, tail(j))
            tails[i] = rest + copy["size"] + HOP
        return tails[i]

    def schedule(known, blocked):
        free, left = {}, list(range(len(copies)))
        while left:
            best = None
            for i in left:
                copy = copies[i]
                needs = [(copy["role"], need) for need in copy["needs"]]
                if all(need in known for need in needs):
                    ready = max(known[need] for need in needs)
                    start = max(free.get((copy["role"], copy["link"]), 0.0), ready)
                    low, high = blocked.get((copy["role"], copy["link"]), (0.0, 0.0))
                    start = high if low < start < high else start
                    key = (round(start, 3), -tail(i), i)
                    if best is None or key < best[0]:
                        best = (key, i, ready)
            (start, _, _), i, ready = best
            copy = copies[i]
            left.remove(i)
            copy["start"], copy["ready"] = start, ready
            free[copy["role"], copy["link"]] = start + copy["size"]
            known[copy["dst"], copy["arrives"]] = start + copy["size"] + HOP
        return known

    def marks(known, role):
        got = [(t, what) for (r, what), t in known.items() if r == role and what[0] == "W"]
        near = max(t for t, what in got if what[2] < 2) + 2.0
        early = max(max(t for t, what in got if what[2] == 2) + 1.8, near + 1.5)
        far = max(max(t for t, what in got) + FAR, early + 0.5)
        return got, near, early, far

    first = schedule(dict(known), {})
    blocked = {}
    for role in "EI":
        gain = marks(first, role)[3] + 1.1
        blocked[role, "x"] = (gain - GUARD, gain + 0.1)
        blocked[role, "z"] = (gain + SECOND - CLEAR, gain + SECOND + 0.1)
    known = schedule(known, blocked)
    steps = {}
    for role in "EI":
        todo = [(0.3, 0, ("norm",))]
        for k, xx in PART_ORDER:
            todo.append((known[role, ("part", k, xx)], 1, ("part", k, xx)))
        got, near, early, far = marks(known, role)
        for t, what in got:
            todo.append((t, 2, what))
        for j in range(3):
            todo.append((near + 0.55 * j, 3, ("dot", 0, j)))
            todo.append((far + 0.55 * (j - 1) if j else early, 3, ("dot", 1, j)))
        gain = marks(first, role)[3] + 1.1
        todo.append((gain, 3, ("gain", 1)))
        todo.append((gain + SECOND, 3, ("gain", 2)))
        for j in range(3):
            todo.append((far + 1.7 + 0.2 * j, 4, ("grad", j)))
        for i, copy in enumerate(copies):
            if copy["role"] == role:
                t = copy["start"] - LEAD
                for link, at in (("x", gain), ("z", gain + SECOND)):
                    if copy["link"] == link and copy["start"] > at:
                        t = max(t, at + 0.01 + copy["start"] / 1000)
                t = 0.0 if copy["needs"] == [("own",)] and t < 1.0 else t
                todo.append((max(copy["ready"], t), 5 + i, ("send", copy)))
        steps[role] = [step for _, _, step in sorted(todo, key=lambda a: a[:2])]
    return steps


def kernel(
    n_z, grad_scale,
    tok_hbm, gain_hbm, w_hbm, kg_hbm,
    tg_ref, wg_ref, gg_ref,
    tok_ref, gain_ref, kg_ref, load_sem, wfull, normed, kgq, inv_ref, inner, dn, part, in1, inz, inx, fin, gsend, grecv, gain_row,
    send_sem, w_recv, c_recv, in1_recv, inz_recv, inx_recv, fin_recv, n_recv, k_recv, g_recv,
):
    rep, grp = lax.axis_index("rep"), lax.axis_index("grp")
    x, c = lax.div(rep, 2), lax.rem(rep, 2)
    z, y = lax.div(grp, 2), lax.rem(grp, 2)
    upper = lax.div(z, 2)
    n_tok, features = tok_ref.shape
    rows, cols = fin.shape
    peer_c = (2 * x + 1 - c, grp)
    peer_x = (2 * (1 - x) + c, grp)
    peer_cx = (2 * (1 - x) + 1 - c, grp)
    peer_y = (rep, 2 * z + 1 - y)
    peer_z = [None] + [(rep, 2 * flip(z, k) + y) for k in range(1, n_z)]
    group = [peer_y]
    for k in range(1, n_z):
        group += [peer_z[k], (rep, 2 * flip(z, k) + 1 - y)]
    bf16, f32 = jnp.bfloat16, jnp.float32

    def row_at(k, yy, h=0, parts=1):
        g = 2 * (k + upper * (3 - 2 * k)) + (1 - y if yy else y)
        return pl.ds(pl.multiple_of(g * rows + h * (rows // parts), 16), rows // parts)

    def col_at(xx):
        r = 2 * (1 - x if xx else x) + c
        return pl.ds(pl.multiple_of(r * cols, LANES), cols)

    own_rows = pl.ds(pl.multiple_of(grp * rows, 16), rows)
    loads = [
        pltpu.make_async_copy(src, dst, load_sem.at[n])
        for n, (src, dst) in enumerate(
            ((w_hbm, wfull.at[own_rows, :]), (tok_hbm, tok_ref), (kg_hbm, kg_ref), (gain_hbm, gain_ref))
        )
    ]
    for load in loads:
        load.start()

    end = lax.rem(lax.div(z + 1, 2), 2) == 0
    inside = jnp.logical_not(end)
    barrier = pltpu.get_barrier_semaphore()
    peers = [peer_c, peer_x, peer_y, peer_z[1]]
    for peer in peers:
        pl.semaphore_signal(barrier, inc=1, device_id=peer, device_id_type=MESH)

    @pl.when(inside)
    def _():
        pl.semaphore_signal(barrier, inc=1, device_id=peer_z[3], device_id_type=MESH)

    pl.semaphore_wait(barrier, len(peers) + inside.astype(jnp.int32))
    loads[0].wait()

    def role(name, steps):
        sends = []

        def send(src, dst, r_sem, peer):
            copy = pltpu.make_async_remote_copy(
                src_ref=src, dst_ref=dst, send_sem=send_sem, recv_sem=r_sem,
                device_id=peer, device_id_type=MESH,
            )
            copy.start()
            sends.append(copy)

        waited = set()

        def arrived(dst, sem, key):
            if key not in waited:
                waited.add(key)
                pltpu.make_async_remote_copy(
                    src_ref=dst, dst_ref=dst, send_sem=sem, recv_sem=sem, device_id=peer_c, device_id_type=MESH
                ).wait_recv()

        def split(h):
            return pl.ds(h * (rows // HR), rows // HR)

        def w_piece(q, k, yy, h):
            return wfull.at[row_at(k, yy, h, HA), col_at(q)]

        def got(what):
            kind = what[0]
            if kind == "W":
                _, q, k, yy, h = what
                arrived(w_piece(q, k, yy, h), w_recv.at[q, k, yy, h], what)
            elif kind == "fin":
                arrived(fin.at[split(what[1]), :], fin_recv.at[what[1]], what)
            elif kind in ("in1", "inz", "inx"):
                _, k, s, h = what
                buf, sem = {"in1": (in1, in1_recv), "inz": (inz, inz_recv), "inx": (inx, inx_recv)}[kind]
                k = k - 1 if kind == "inz" and k else k
                arrived(buf.at[k, s, split(h), :], sem.at[k, s, h], what)

        def kept(k, s, h):
            return (k, s, 0, split(h), slice(None)) if (k, h) in XF else (k, 0, s, split(h), slice(None))

        def given(k, s, h):
            return (k, s, 1, split(h), slice(None)) if (k, h) in XF else (k, 1, s, split(h), slice(None))

        def summed(k, s, h):
            at = split(h)
            total = part[kept(k, s, h)].astype(f32)
            terms = [("in1", in1)]
            if name == "E":
                terms += [("inz", inz)] if k == 0 else []
            else:
                terms += ([("inz", inz)] if k > 0 else []) + ([("inx", inx)] if k < 2 else [])
            for kind, buf in terms:
                got((kind, k, s, h))
                slot = k - 1 if kind == "inz" and k else k
                total = total + buf[slot, s, at, :].astype(f32)
            return total

        def send_copy(copy):
            what, arrives, link = copy["what"], copy["arrives"], copy["link"]
            peer = {"x": peer_x, "y": peer_y, "z": peer_z[1], "across": peer_z[3]}[link]
            for need in copy["needs"]:
                got(need)
            if what[0] == "W":
                _, q, k, yy, h = what
                piece = w_piece(q, k, yy, h)
                send(piece, piece, w_recv.at[arrives[1:]], peer)
                return
            if arrives[0] == "fin":
                dst, sem = fin.at[split(arrives[1]), :], fin_recv.at[arrives[1]]
            else:
                _, k, s, h = arrives
                buf, sems = {"in1": (in1, in1_recv), "inz": (inz, inz_recv), "inx": (inx, inx_recv)}[arrives[0]]
                k = k - 1 if arrives[0] == "inz" and k else k
                dst, sem = buf.at[k, s, split(h), :], sems.at[k, s, h]
            _, k, s, h = what
            if what[0] == "one":
                send(part.at[given(k, s, h)], dst, sem, peer)
            else:
                part[kept(k, s, h)] = summed(k, s, h).astype(bf16)
                send(part.at[kept(k, s, h)], dst, sem, peer)

        def norm():
            loads[2].wait()
            for xx in (1, 0):
                theirs = pl.ds(pl.multiple_of((2 * (1 - x if xx else x) + 1 - c) * cols, LANES), cols)
                send(kg_ref.at[:, theirs], kgq.at[xx, pl.ds(n_tok, n_tok), :], k_recv, peer_c)
            loads[1].wait()
            acc = None
            for j in range(features // LANES):
                t = tok_ref[:, j * LANES:(j + 1) * LANES].astype(f32)
                acc = t * t if acc is None else acc + t * t
            inv = lax.rsqrt(jnp.sum(acc, axis=1, keepdims=True) / features + epsilon)
            inv_ref[...] = inv
            inner[...] = jnp.zeros_like(inner)
            loads[3].wait()
            for j in range(features // LANES):
                at = slice(j * LANES, (j + 1) * LANES)
                gain_row[:, at] = gain_ref[at].reshape(1, -1)
            half = features // 2
            for far in (1, 0):
                for j in range(half // LANES):
                    base = (1 - upper if far else upper) * half + j * LANES
                    at = pl.ds(pl.multiple_of(base, LANES), LANES)
                    t = tok_ref[:, at].astype(f32)
                    normed[at, :n_tok] = (t * inv * gain_row[:, at]).T.astype(bf16)
                for k in (3, 2) if far else (0, 1):
                    send(normed.at[pair_at(k), pl.ds(0, n_tok)], theirs_at(k), n_recv.at[k], peer_c)
            for xx in (0, 1):
                kgq[xx, :n_tok, :] = kg_ref[:, col_at(xx)]

        def pair_at(k):
            return pl.ds(pl.multiple_of(2 * rows * (k + upper * (3 - 2 * k)), 16), 2 * rows)

        def theirs_at(k):
            return normed.at[pair_at(k), pl.ds(n_tok, n_tok)]

        def block(k, xx):
            arrived(kgq.at[:, pl.ds(n_tok, n_tok), :], k_recv, "kg")
            arrived(theirs_at(k), n_recv.at[k], ("normed", k))
            both = jnp.dot(normed[pair_at(k), :], kgq[xx], preferred_element_type=f32).astype(bf16)
            part[k, y, xx] = both[:rows]
            part[k, 1 - y, xx] = both[rows:]

        me = 0 if name == "E" else 1

        def dots(far, j):
            for k in ([0, 1] if j == 0 else []) if not far else [2 if j == 0 else 3]:
                shards = [yy for yy in (0, 1) if (k, yy) != (me, 0)]
                for yy in shards:
                    for q in (0, 1):
                        for h in range(HA):
                            got(("W", q, k, yy, h))
                amount = wfull.at[pl.ds(0, len(shards) * rows), pl.ds(0, 2 * cols)]
                arrived(amount, c_recv.at[k], ("C", k))
            wide = features // 6
            side = 1 - upper if far else upper
            base = side * (features // 2) + (j + upper * (2 - 2 * j)) * wide
            at = pl.ds(pl.multiple_of(base, LANES), wide)
            d = lax.dot_general(
                kg_ref[...], wfull[at, :], (((1,), (1,)), ((), ())), preferred_element_type=f32
            )
            dn[:, at] = d
            dt = d * tok_ref[:, at].astype(f32)
            gsend[0, :, at] = jnp.sum(dt * inv_ref[...], axis=0, keepdims=True)
            gain_at = gain_row[:, at]
            scaled = dt * gain_at
            add = scaled[:, :LANES]
            for n in range(1, wide // LANES):
                add = add + scaled[:, n * LANES:(n + 1) * LANES]
            inner[...] = inner[...] + add

        def gain(stage):
            if stage == 1:
                for n, peer in enumerate((peer_c, peer_x, peer_cx)):
                    send(gsend.at[0], grecv.at[n], g_recv.at[0], peer)
                return
            arrived(grecv.at[pl.ds(0, 3)], g_recv.at[0], "g0")
            gsend[1] = (gsend[0] + grecv[0]) + (grecv[1] + grecv[2])
            for n, peer in reversed(list(enumerate(group))):
                send(gsend.at[1], grecv.at[3 + n], g_recv.at[1], peer)

        def grad(j):
            inv = inv_ref[...]
            pull = inv * inv * (jnp.sum(inner[...], axis=1, keepdims=True) / features)
            wide = features // 9
            for n in range(3 * j, 3 * j + 3):
                at = slice(n * wide, (n + 1) * wide)
                t = tok_ref[:, at].astype(f32)
                tg_ref[:, at] = (inv * (dn[:, at] * gain_ref[at].reshape(1, -1) - t * pull)).astype(bf16)

        for step in steps:
            kind = step[0]
            if kind == "send":
                send_copy(step[1])
            elif kind == "norm":
                norm()
            elif kind == "part":
                block(*step[1:])
            elif kind == "W":
                _, q, k, yy, h = step
                got(step)
                piece = w_piece(q, k, yy, h)
                send(piece, piece, c_recv.at[k], peer_c)
            elif kind == "dot":
                dots(*step[1:])
            elif kind == "gain":
                gain(step[1])
            else:
                grad(step[1])

        for h in range(HR):
            total = summed(me, 0, h)
            got(("fin", h))
            wg_ref[split(h), :] = (total + fin[split(h), :].astype(f32)) * grad_scale
        terms = [gsend[1]]
        arrived(grecv.at[pl.ds(3, len(group))], g_recv.at[1], "g1")
        for n in range(3, 3 + len(group)):
            terms.append(grecv[n])
        while len(terms) > 1:
            terms = [terms[i] + terms[i + 1] for i in range(0, len(terms), 2)]
        total = terms[0] * grad_scale
        for j in range(features // LANES):
            at = slice(j * LANES, (j + 1) * LANES)
            gg_ref[at] = total[:, at].reshape(LANES)
        for copy in sends:
            copy.wait_send()

    steps = plan()
    for name, here in (("E", end), ("I", inside)):
        pl.when(here)(functools.partial(role, name, steps[name]))


def drain(tg_ref, wg_ref, gg_ref, tg_out, wg_out, gg_out, sem):
    copies = [
        pltpu.make_async_copy(src, dst, sem.at[n])
        for n, (src, dst) in enumerate(((tg_ref, tg_out), (wg_ref, wg_out), (gg_ref, gg_out)))
    ]
    for copy in copies:
        copy.start()
    for copy in copies:
        copy.wait()


def fused(n_rep, n_grp, tokens, norm_gain, key_weight, key_grad):
    n_tok, features = tokens.shape
    rows, keys = key_weight.shape
    cols, n_z = keys // n_rep, n_grp // 2
    grad_scale = (n_tok * n_rep * n_grp) ** (-0.5)
    vmem = pl.BlockSpec(memory_space=pltpu.VMEM)
    bf16, f32, dma = jnp.bfloat16, jnp.float32, pltpu.SemaphoreType.DMA
    block = (rows, cols)
    token_grad, weight_grad, gain_grad = pl.pallas_call(
        functools.partial(kernel, n_z, grad_scale),
        out_shape=(
            jax.ShapeDtypeStruct((n_tok, features), bf16),
            jax.ShapeDtypeStruct(block, f32),
            jax.ShapeDtypeStruct((features,), f32),
        ),
        in_specs=[pl.BlockSpec(memory_space=pltpu.HBM)] * 4,
        out_specs=(vmem,) * 3,
        scratch_shapes=[
            pltpu.VMEM((n_tok, features), bf16),
            pltpu.VMEM((features,), f32),
            pltpu.VMEM((n_tok, keys), bf16),
            dma((4,)),
            pltpu.VMEM((features, keys), bf16),
            pltpu.VMEM((features, 2 * n_tok), bf16),
            pltpu.VMEM((2, 2 * n_tok, cols), bf16),
            pltpu.VMEM((n_tok, 1), f32),
            pltpu.VMEM((n_tok, LANES), f32),
            pltpu.VMEM((n_tok, features), f32),
            pltpu.VMEM((n_z, 2, 2) + block, bf16),
            pltpu.VMEM((n_z, 2) + block, bf16),
            pltpu.VMEM((n_z - 1, 2) + block, bf16),
            pltpu.VMEM((2, 2) + block, bf16),
            pltpu.VMEM(block, bf16),
            pltpu.VMEM((2, 1, features), f32),
            pltpu.VMEM((2 * n_z + 2, 1, features), f32),
            pltpu.VMEM((1, features), f32),
            dma, dma((2, n_z, 2, HA)), dma((n_z,)),
            dma((n_z, 2, HR)), dma((n_z - 1, 2, HR)), dma((2, 2, HR)), dma((HR,)),
            dma((n_z,)), dma, dma((2,)),
        ],
        compiler_params=pltpu.CompilerParams(
            collective_id=0, has_side_effects=True, vmem_limit_bytes=40 * 1024 * 1024
        ),
    )(*(pltpu.with_memory_space_constraint(a, pltpu.MemorySpace.HBM) for a in (tokens, norm_gain, key_weight, key_grad)))
    return pl.pallas_call(
        drain,
        out_shape=tuple(jax.ShapeDtypeStruct(a.shape, a.dtype) for a in (token_grad, weight_grad, gain_grad)),
        in_specs=[vmem] * 3,
        out_specs=(pl.BlockSpec(memory_space=pl.ANY),) * 3,
        scratch_shapes=[dma((3,))],
        compiler_params=pltpu.CompilerParams(vmem_limit_bytes=8 * 1024 * 1024),
    )(token_grad, weight_grad, gain_grad)


def plain(tokens, norm_gain, key_weight, key_grad):
    total_tokens = tokens.shape[0] * lax.axis_size("rep") * lax.axis_size("grp")
    grad_scale = total_tokens ** (-0.5)
    wide_tokens = tokens.astype(jnp.float32)
    inv_rms = lax.rsqrt(jnp.mean(wide_tokens * wide_tokens, axis=1, keepdims=True) + epsilon)
    normed = (wide_tokens * inv_rms * norm_gain).astype(jnp.bfloat16)
    partial_value = lax.dot_general(
        normed, key_grad, (((0,), (0,)), ((), ())), preferred_element_type=jnp.float32
    )
    d_normed = lax.dot_general(
        key_grad,
        lax.all_gather(key_weight, "grp", axis=0, tiled=True),
        (((1,), (1,)), ((), ())),
        preferred_element_type=jnp.float32,
    )
    section_one = lax.psum_scatter(
        partial_value.astype(jnp.bfloat16), "rep", scatter_dimension=1, tiled=True
    ).astype(jnp.float32)
    weight_sum = lax.psum_scatter(section_one, "grp", scatter_dimension=0, tiled=True)
    gain_local = jnp.sum(d_normed * wide_tokens * inv_rms, axis=0)
    gain_total = lax.psum(gain_local, ("rep", "grp"))
    scaled = d_normed * norm_gain
    inner_mean = jnp.mean(scaled * wide_tokens, axis=1, keepdims=True)
    token_grad = (inv_rms * (scaled - wide_tokens * inv_rms * inv_rms * inner_mean)).astype(
        jnp.bfloat16
    )
    return (token_grad, weight_sum * grad_scale, gain_total * grad_scale)


def shards(tokens, norm_gain, key_weight, key_grad):
    n_rep, n_grp = lax.axis_size("rep"), lax.axis_size("grp")
    n_z = n_grp // 2
    if (
        n_rep == 2 * 2 and n_grp == 2 * 4
        and key_weight.shape[1] % (n_rep * LANES) == 0 and key_weight.shape[0] % 96 == 0
        and tokens.shape[1] % (18 * LANES) == 0 and tokens.shape[0] % LANES == 0
    ):
        return fused(n_rep, n_grp, tokens, norm_gain, key_weight, key_grad)
    return plain(tokens, norm_gain, key_weight, key_grad)


def solution(mesh):
    in_specs = (P(("rep", "grp"), None), P(), P("grp", None), P(("rep", "grp"), None))
    out_specs = (P(("rep", "grp"), None), P("grp", "rep"), P())
    return jax.shard_map(shards, mesh=mesh, in_specs=in_specs, out_specs=out_specs, check_vma=False)
```

```python
import functools

import jax
import jax.numpy as jnp
from jax import lax
from jax.experimental import pallas as pl
from jax.experimental.pallas import tpu as pltpu
from jax.sharding import PartitionSpec as P

epsilon = 1e-06
MESH = pl.DeviceIdType.MESH
LANES = 128


def flip(i, bits):
    bit = 1
    while bit <= bits:
        if bits & bit:
            i = i + bit * (1 - 2 * lax.rem(lax.div(i, bit), 2))
        bit *= 2
    return i


HA, HR = 2, 3
PIECE, HOP, LEAD, AHEAD = 3.2, 2.5, 1.2, 11.0
OWN, PART, STEP, GUARD = 0.4, 2.7, 0.45, 0.6
SECOND, CLEAR, EDGE = 2.8, 0.4, 2.0
FAR, AGT, RST = 1.4, 1.0, 1.5
XF = {(0, 0), (0, 1), (1, 0), (1, 1), (2, 0), (2, 1), (3, 0), (3, 1)}
BY_Y = {"E": {(3, 0), (3, 1)}, "I": {(3, 0), (3, 1)}}
PART_ORDER = [(3, 1), (2, 1), (2, 0), (3, 0), (0, 1), (1, 1), (1, 0), (0, 0)]


def messages():
    out = []

    def add(role, link, what, dst, arrives, needs, size):
        out.append(dict(role=role, link=link, what=what, dst=dst, arrives=arrives, needs=needs, size=size))

    for h in range(HA):
        size = PIECE / HA
        for role, me in (("E", 0), ("I", 1)):
            for q in (0, 1):
                for k in range(4):
                    needs = ("own",) if k == me else ("W", q, k, 0, h)
                    if q == 0:
                        add(role, "y", ("W", q, k, 0, h), role, ("W", q, k, 1, h), [needs], size)
                        if (k, h) not in BY_Y[role]:
                            add(role, "x", ("W", q, k, 1, h), role, ("W", 1, k, 1, h), [("W", 0, k, 1, h)], size)
                    elif (k, h) in BY_Y[role]:
                        add(role, "y", ("W", q, k, 0, h), role, ("W", 1, k, 1, h), [needs], size)
                    if role == "E" and k == 0:
                        add(role, "z", ("W", q, k, 0, h), "I", ("W", q, 0, 0, h), [needs], size)
                    if role == "I" and k >= 1:
                        add(role, "z", ("W", q, k, 0, h), "E", ("W", q, k, 0, h), [needs], size)
                    if role == "I" and k <= 1:
                        add(role, "across", ("W", q, k, 0, h), "I", ("W", q, 3 - k, 0, h), [needs], size)
    for h in range(HR):
        size = PIECE / HR
        for s in (0, 1):
            for role in "EI":
                for k in range(4):
                    first = (k, h) in XF
                    link, needs = ("x", ("part", k, 1)) if first else ("y", ("part", k, s))
                    add(role, link, ("one", k, s, h), role, ("in1", k, s, h), [needs], size)
            kept = [("part", k, 0 if (k, h) in XF else s) for k in range(4)]
            for k in (1, 2, 3):
                needs = [kept[k], ("in1", k, s, h)]
                add("E", "z", ("sum", k, s, h), "I", ("inz", k, s, h), needs, size)
                if k > 1:
                    needs = needs + [("inz", k, s, h)]
                    add("I", "across", ("sum", k, s, h), "I", ("inx", 3 - k, s, h), needs, size)
            needs = [kept[0], ("in1", 0, s, h), ("inx", 0, s, h)]
            add("I", "z", ("sum", 0, s, h), "E", ("inz", 0, s, h), needs, size)
        for role, k in (("E", 0), ("I", 1)):
            needs = [kept[k], ("in1", k, 1, h), ("inz", k, 1, h)] + ([("inx", 1, 1, h)] if k else [])
            add(role, "y" if (k, h) in XF else "x", ("sum", k, 1, h), role, ("fin", h), needs, size)
    return out


def plan():
    copies = messages()
    known, users, tails = {}, {}, {}
    for role in "EI":
        known[role, ("own",)] = OWN
        for i, (k, xx) in enumerate(PART_ORDER):
            known[role, ("part", k, xx)] = PART + STEP * i
    for i, copy in enumerate(copies):
        for need in copy["needs"]:
            users.setdefault((copy["role"], need), []).append(i)

    def tail(i):
        if i not in tails:
            copy = copies[i]
            rest = {"W": AHEAD, "fin": RST + (EDGE if copy["dst"] == "E" else 0.0)}.get(copy["arrives"][0], RST)
            for j in users.get((copy["dst"], copy["arrives"]), []):
                rest = max(rest, tail(j))
            tails[i] = rest + copy["size"] + HOP
        return tails[i]

    def schedule(known, blocked):
        free, left = {}, list(range(len(copies)))
        while left:
            best = None
            for i in left:
                copy = copies[i]
                needs = [(copy["role"], need) for need in copy["needs"]]
                if all(need in known for need in needs):
                    ready = max(known[need] for need in needs)
                    start = max(free.get((copy["role"], copy["link"]), 0.0), ready)
                    low, high = blocked.get((copy["role"], copy["link"]), (0.0, 0.0))
                    start = high if low < start < high else start
                    key = (round(start, 3), -tail(i), i)
                    if best is None or key < best[0]:
                        best = (key, i, ready)
            (start, _, _), i, ready = best
            copy = copies[i]
            left.remove(i)
            copy["start"], copy["ready"] = start, ready
            free[copy["role"], copy["link"]] = start + copy["size"]
            known[copy["dst"], copy["arrives"]] = start + copy["size"] + HOP
        return known

    def marks(known, role):
        got = [(t, what) for (r, what), t in known.items() if r == role and what[0] == "W"]
        near = max(t for t, what in got if what[2] < 2) + 2.0
        early = max(max(t for t, what in got if what[2] == 2) + 1.8, near + 1.5)
        far = max(max(t for t, what in got) + FAR, early + 0.5)
        return got, near, early, far

    first = schedule(dict(known), {})
    blocked = {}
    for role in "EI":
        gain = marks(first, role)[3] + 1.1
        blocked[role, "x"] = (gain - GUARD, gain + 0.1)
        blocked[role, "z"] = (gain + SECOND - CLEAR, gain + SECOND + 0.1)
    known = schedule(known, blocked)
    steps = {}
    for role in "EI":
        todo = [(0.3, 0, ("norm",))]
        for k, xx in PART_ORDER:
            todo.append((known[role, ("part", k, xx)], 1, ("part", k, xx)))
        got, near, early, far = marks(known, role)
        for t, what in got:
            todo.append((t, 2, what))
        for j in range(3):
            todo.append((near + 0.55 * j, 3, ("dot", 0, j)))
            todo.append((far + 0.55 * (j - 1) if j else early, 3, ("dot", 1, j)))
        gain = marks(first, role)[3] + 1.1
        todo.append((gain, 3, ("gain", 1)))
        todo.append((gain + SECOND, 3, ("gain", 2)))
        for j in range(3):
            todo.append((far + 1.7 + 0.2 * j, 4, ("grad", j)))
        for i, copy in enumerate(copies):
            if copy["role"] == role:
                t = copy["start"] - LEAD
                for link, at in (("x", gain), ("z", gain + SECOND)):
                    if copy["link"] == link and copy["start"] > at:
                        t = max(t, at + 0.01 + copy["start"] / 1000)
                t = 0.0 if copy["needs"] == [("own",)] and t < 1.0 else t
                todo.append((max(copy["ready"], t), 5 + i, ("send", copy)))
        steps[role] = [step for _, _, step in sorted(todo, key=lambda a: a[:2])]
    return steps


def kernel(
    n_z, grad_scale,
    tok_hbm, gain_hbm, w_hbm, kg_hbm,
    tg_ref, wg_ref, gg_ref,
    tok_ref, gain_ref, kg_ref, load_sem, wfull, normed, kgq, inv_ref, inner, dn, part, in1, inz, inx, fin, gsend, grecv, gain_row,
    send_sem, w_recv, c_recv, in1_recv, inz_recv, inx_recv, fin_recv, n_recv, k_recv, g_recv,
):
    rep, grp = lax.axis_index("rep"), lax.axis_index("grp")
    x, c = lax.div(rep, 2), lax.rem(rep, 2)
    z, y = lax.div(grp, 2), lax.rem(grp, 2)
    upper = lax.div(z, 2)
    n_tok, features = tok_ref.shape
    rows, cols = fin.shape
    peer_c = (2 * x + 1 - c, grp)
    peer_x = (2 * (1 - x) + c, grp)
    peer_cx = (2 * (1 - x) + 1 - c, grp)
    peer_y = (rep, 2 * z + 1 - y)
    peer_z = [None] + [(rep, 2 * flip(z, k) + y) for k in range(1, n_z)]
    group = [peer_y]
    for k in range(1, n_z):
        group += [peer_z[k], (rep, 2 * flip(z, k) + 1 - y)]
    bf16, f32 = jnp.bfloat16, jnp.float32

    def row_at(k, yy, h=0, parts=1):
        g = 2 * (k + upper * (3 - 2 * k)) + (1 - y if yy else y)
        return pl.ds(pl.multiple_of(g * rows + h * (rows // parts), 16), rows // parts)

    def col_at(xx):
        r = 2 * (1 - x if xx else x) + c
        return pl.ds(pl.multiple_of(r * cols, LANES), cols)

    own_rows = pl.ds(pl.multiple_of(grp * rows, 16), rows)
    loads = [
        pltpu.make_async_copy(src, dst, load_sem.at[n])
        for n, (src, dst) in enumerate(
            ((w_hbm, wfull.at[own_rows, :]), (tok_hbm, tok_ref), (kg_hbm, kg_ref), (gain_hbm, gain_ref))
        )
    ]
    for load in (loads[1], loads[0], loads[2], loads[3]):
        load.start()

    end = lax.rem(lax.div(z + 1, 2), 2) == 0
    inside = jnp.logical_not(end)
    barrier = pltpu.get_barrier_semaphore()
    peers = [peer_c, peer_x, peer_y, peer_z[1]]
    for peer in peers:
        pl.semaphore_signal(barrier, inc=1, device_id=peer, device_id_type=MESH)

    @pl.when(inside)
    def _():
        pl.semaphore_signal(barrier, inc=1, device_id=peer_z[3], device_id_type=MESH)

    pl.semaphore_wait(barrier, len(peers) + inside.astype(jnp.int32))
    loads[0].wait()

    def role(name, steps):
        sends = []

        def send(src, dst, r_sem, peer):
            copy = pltpu.make_async_remote_copy(
                src_ref=src, dst_ref=dst, send_sem=send_sem, recv_sem=r_sem,
                device_id=peer, device_id_type=MESH,
            )
            copy.start()
            sends.append(copy)

        waited = set()

        def arrived(dst, sem, key):
            if key not in waited:
                waited.add(key)
                pltpu.make_async_remote_copy(
                    src_ref=dst, dst_ref=dst, send_sem=sem, recv_sem=sem, device_id=peer_c, device_id_type=MESH
                ).wait_recv()

        def split(h):
            return pl.ds(h * (rows // HR), rows // HR)

        def w_piece(q, k, yy, h):
            return wfull.at[row_at(k, yy, h, HA), col_at(q)]

        def got(what):
            kind = what[0]
            if kind == "W":
                _, q, k, yy, h = what
                arrived(w_piece(q, k, yy, h), w_recv.at[q, k, yy, h], what)
            elif kind == "fin":
                arrived(fin.at[split(what[1]), :], fin_recv.at[what[1]], what)
            elif kind in ("in1", "inz", "inx"):
                _, k, s, h = what
                buf, sem = {"in1": (in1, in1_recv), "inz": (inz, inz_recv), "inx": (inx, inx_recv)}[kind]
                k = k - 1 if kind == "inz" and k else k
                arrived(buf.at[k, s, split(h), :], sem.at[k, s, h], what)

        def kept(k, s, h):
            return (k, s, 0, split(h), slice(None)) if (k, h) in XF else (k, 0, s, split(h), slice(None))

        def given(k, s, h):
            return (k, s, 1, split(h), slice(None)) if (k, h) in XF else (k, 1, s, split(h), slice(None))

        def summed(k, s, h):
            at = split(h)
            total = part[kept(k, s, h)].astype(f32)
            terms = [("in1", in1)]
            if name == "E":
                terms += [("inz", inz)] if k == 0 else []
            else:
                terms += ([("inz", inz)] if k > 0 else []) + ([("inx", inx)] if k < 2 else [])
            for kind, buf in terms:
                got((kind, k, s, h))
                slot = k - 1 if kind == "inz" and k else k
                total = total + buf[slot, s, at, :].astype(f32)
            return total

        def send_copy(copy):
            what, arrives, link = copy["what"], copy["arrives"], copy["link"]
            peer = {"x": peer_x, "y": peer_y, "z": peer_z[1], "across": peer_z[3]}[link]
            for need in copy["needs"]:
                got(need)
            if what[0] == "W":
                _, q, k, yy, h = what
                piece = w_piece(q, k, yy, h)
                send(piece, piece, w_recv.at[arrives[1:]], peer)
                return
            if arrives[0] == "fin":
                dst, sem = fin.at[split(arrives[1]), :], fin_recv.at[arrives[1]]
            else:
                _, k, s, h = arrives
                buf, sems = {"in1": (in1, in1_recv), "inz": (inz, inz_recv), "inx": (inx, inx_recv)}[arrives[0]]
                k = k - 1 if arrives[0] == "inz" and k else k
                dst, sem = buf.at[k, s, split(h), :], sems.at[k, s, h]
            _, k, s, h = what
            if what[0] == "one":
                send(part.at[given(k, s, h)], dst, sem, peer)
            else:
                part[kept(k, s, h)] = summed(k, s, h).astype(bf16)
                send(part.at[kept(k, s, h)], dst, sem, peer)

        def norm():
            loads[2].wait()
            for xx in (1, 0):
                theirs = pl.ds(pl.multiple_of((2 * (1 - x if xx else x) + 1 - c) * cols, LANES), cols)
                send(kg_ref.at[:, theirs], kgq.at[xx, pl.ds(n_tok, n_tok), :], k_recv, peer_c)
            loads[1].wait()
            acc = None
            for j in range(features // LANES):
                t = tok_ref[:, j * LANES:(j + 1) * LANES].astype(f32)
                acc = t * t if acc is None else acc + t * t
            inv = lax.rsqrt(jnp.sum(acc, axis=1, keepdims=True) / features + epsilon)
            inv_ref[...] = inv
            inner[...] = jnp.zeros_like(inner)
            loads[3].wait()
            for j in range(features // LANES):
                at = slice(j * LANES, (j + 1) * LANES)
                gain_row[:, at] = gain_ref[at].reshape(1, -1)
            half = features // 2
            for far in (1, 0):
                for j in range(half // LANES):
                    base = (1 - upper if far else upper) * half + j * LANES
                    at = pl.ds(pl.multiple_of(base, LANES), LANES)
                    t = tok_ref[:, at].astype(f32)
                    normed[at, :n_tok] = (t * inv * gain_row[:, at]).T.astype(bf16)
                for k in (3, 2) if far else (0, 1):
                    send(normed.at[pair_at(k), pl.ds(0, n_tok)], theirs_at(k), n_recv.at[k], peer_c)
            for xx in (0, 1):
                kgq[xx, :n_tok, :] = kg_ref[:, col_at(xx)]

        def pair_at(k):
            return pl.ds(pl.multiple_of(2 * rows * (k + upper * (3 - 2 * k)), 16), 2 * rows)

        def theirs_at(k):
            return normed.at[pair_at(k), pl.ds(n_tok, n_tok)]

        def block(k, xx):
            arrived(kgq.at[:, pl.ds(n_tok, n_tok), :], k_recv, "kg")
            arrived(theirs_at(k), n_recv.at[k], ("normed", k))
            both = jnp.dot(normed[pair_at(k), :], kgq[xx], preferred_element_type=f32).astype(bf16)
            part[k, y, xx] = both[:rows]
            part[k, 1 - y, xx] = both[rows:]

        me = 0 if name == "E" else 1

        def dots(far, j):
            for k in ([0, 1] if j == 0 else []) if not far else [2 if j == 0 else 3]:
                shards = [yy for yy in (0, 1) if (k, yy) != (me, 0)]
                for yy in shards:
                    for q in (0, 1):
                        for h in range(HA):
                            got(("W", q, k, yy, h))
                amount = wfull.at[pl.ds(0, len(shards) * rows), pl.ds(0, 2 * cols)]
                arrived(amount, c_recv.at[k], ("C", k))
            wide = features // 6
            side = 1 - upper if far else upper
            base = side * (features // 2) + (j + upper * (2 - 2 * j)) * wide
            at = pl.ds(pl.multiple_of(base, LANES), wide)
            d = lax.dot_general(
                kg_ref[...], wfull[at, :], (((1,), (1,)), ((), ())), preferred_element_type=f32
            )
            dn[:, at] = d
            dt = d * tok_ref[:, at].astype(f32)
            gsend[0, :, at] = jnp.sum(dt * inv_ref[...], axis=0, keepdims=True)
            gain_at = gain_row[:, at]
            scaled = dt * gain_at
            add = scaled[:, :LANES]
            for n in range(1, wide // LANES):
                add = add + scaled[:, n * LANES:(n + 1) * LANES]
            inner[...] = inner[...] + add

        def gain(stage):
            if stage == 1:
                for n, peer in enumerate((peer_c, peer_x, peer_cx)):
                    send(gsend.at[0], grecv.at[n], g_recv.at[0], peer)
                return
            arrived(grecv.at[pl.ds(0, 3)], g_recv.at[0], "g0")
            gsend[1] = (gsend[0] + grecv[0]) + (grecv[1] + grecv[2])
            for n, peer in reversed(list(enumerate(group))):
                send(gsend.at[1], grecv.at[3 + n], g_recv.at[1], peer)

        def grad(j):
            inv = inv_ref[...]
            pull = inv * inv * (jnp.sum(inner[...], axis=1, keepdims=True) / features)
            wide = features // 9
            for n in range(3 * j, 3 * j + 3):
                at = slice(n * wide, (n + 1) * wide)
                t = tok_ref[:, at].astype(f32)
                tg_ref[:, at] = (inv * (dn[:, at] * gain_ref[at].reshape(1, -1) - t * pull)).astype(bf16)

        for step in steps:
            kind = step[0]
            if kind == "send":
                send_copy(step[1])
            elif kind == "norm":
                norm()
            elif kind == "part":
                block(*step[1:])
            elif kind == "W":
                _, q, k, yy, h = step
                got(step)
                piece = w_piece(q, k, yy, h)
                send(piece, piece, c_recv.at[k], peer_c)
            elif kind == "dot":
                dots(*step[1:])
            elif kind == "gain":
                gain(step[1])
            else:
                grad(step[1])

        for h in range(HR):
            total = summed(me, 0, h)
            got(("fin", h))
            wg_ref[split(h), :] = (total + fin[split(h), :].astype(f32)) * grad_scale
        terms = [gsend[1]]
        arrived(grecv.at[pl.ds(3, len(group))], g_recv.at[1], "g1")
        for n in range(3, 3 + len(group)):
            terms.append(grecv[n])
        while len(terms) > 1:
            terms = [terms[i] + terms[i + 1] for i in range(0, len(terms), 2)]
        total = terms[0] * grad_scale
        for j in range(features // LANES):
            at = slice(j * LANES, (j + 1) * LANES)
            gg_ref[at] = total[:, at].reshape(LANES)
        for copy in sends:
            copy.wait_send()

    steps = plan()
    for name, here in (("E", end), ("I", inside)):
        pl.when(here)(functools.partial(role, name, steps[name]))


def drain(tg_ref, wg_ref, gg_ref, tg_out, wg_out, gg_out, sem):
    copies = [
        pltpu.make_async_copy(src, dst, sem.at[n])
        for n, (src, dst) in enumerate(((tg_ref, tg_out), (wg_ref, wg_out), (gg_ref, gg_out)))
    ]
    for copy in copies:
        copy.start()
    for copy in copies:
        copy.wait()


def fused(n_rep, n_grp, tokens, norm_gain, key_weight, key_grad):
    n_tok, features = tokens.shape
    rows, keys = key_weight.shape
    cols, n_z = keys // n_rep, n_grp // 2
    grad_scale = (n_tok * n_rep * n_grp) ** (-0.5)
    vmem = pl.BlockSpec(memory_space=pltpu.VMEM)
    bf16, f32, dma = jnp.bfloat16, jnp.float32, pltpu.SemaphoreType.DMA
    block = (rows, cols)
    token_grad, weight_grad, gain_grad = pl.pallas_call(
        functools.partial(kernel, n_z, grad_scale),
        out_shape=(
            jax.ShapeDtypeStruct((n_tok, features), bf16),
            jax.ShapeDtypeStruct(block, f32),
            jax.ShapeDtypeStruct((features,), f32),
        ),
        in_specs=[pl.BlockSpec(memory_space=pltpu.HBM)] * 4,
        out_specs=(vmem,) * 3,
        scratch_shapes=[
            pltpu.VMEM((n_tok, features), bf16),
            pltpu.VMEM((features,), f32),
            pltpu.VMEM((n_tok, keys), bf16),
            dma((4,)),
            pltpu.VMEM((features, keys), bf16),
            pltpu.VMEM((features, 2 * n_tok), bf16),
            pltpu.VMEM((2, 2 * n_tok, cols), bf16),
            pltpu.VMEM((n_tok, 1), f32),
            pltpu.VMEM((n_tok, LANES), f32),
            pltpu.VMEM((n_tok, features), f32),
            pltpu.VMEM((n_z, 2, 2) + block, bf16),
            pltpu.VMEM((n_z, 2) + block, bf16),
            pltpu.VMEM((n_z - 1, 2) + block, bf16),
            pltpu.VMEM((2, 2) + block, bf16),
            pltpu.VMEM(block, bf16),
            pltpu.VMEM((2, 1, features), f32),
            pltpu.VMEM((2 * n_z + 2, 1, features), f32),
            pltpu.VMEM((1, features), f32),
            dma, dma((2, n_z, 2, HA)), dma((n_z,)),
            dma((n_z, 2, HR)), dma((n_z - 1, 2, HR)), dma((2, 2, HR)), dma((HR,)),
            dma((n_z,)), dma, dma((2,)),
        ],
        compiler_params=pltpu.CompilerParams(
            collective_id=0, has_side_effects=True, vmem_limit_bytes=40 * 1024 * 1024
        ),
    )(*(pltpu.with_memory_space_constraint(a, pltpu.MemorySpace.HBM) for a in (tokens, norm_gain, key_weight, key_grad)))
    return pl.pallas_call(
        drain,
        out_shape=tuple(jax.ShapeDtypeStruct(a.shape, a.dtype) for a in (token_grad, weight_grad, gain_grad)),
        in_specs=[vmem] * 3,
        out_specs=(pl.BlockSpec(memory_space=pl.ANY),) * 3,
        scratch_shapes=[dma((3,))],
        compiler_params=pltpu.CompilerParams(vmem_limit_bytes=8 * 1024 * 1024),
    )(token_grad, weight_grad, gain_grad)


def plain(tokens, norm_gain, key_weight, key_grad):
    total_tokens = tokens.shape[0] * lax.axis_size("rep") * lax.axis_size("grp")
    grad_scale = total_tokens ** (-0.5)
    wide_tokens = tokens.astype(jnp.float32)
    inv_rms = lax.rsqrt(jnp.mean(wide_tokens * wide_tokens, axis=1, keepdims=True) + epsilon)
    normed = (wide_tokens * inv_rms * norm_gain).astype(jnp.bfloat16)
    partial_value = lax.dot_general(
        normed, key_grad, (((0,), (0,)), ((), ())), preferred_element_type=jnp.float32
    )
    d_normed = lax.dot_general(
        key_grad,
        lax.all_gather(key_weight, "grp", axis=0, tiled=True),
        (((1,), (1,)), ((), ())),
        preferred_element_type=jnp.float32,
    )
    section_one = lax.psum_scatter(
        partial_value.astype(jnp.bfloat16), "rep", scatter_dimension=1, tiled=True
    ).astype(jnp.float32)
    weight_sum = lax.psum_scatter(section_one, "grp", scatter_dimension=0, tiled=True)
    gain_local = jnp.sum(d_normed * wide_tokens * inv_rms, axis=0)
    gain_total = lax.psum(gain_local, ("rep", "grp"))
    scaled = d_normed * norm_gain
    inner_mean = jnp.mean(scaled * wide_tokens, axis=1, keepdims=True)
    token_grad = (inv_rms * (scaled - wide_tokens * inv_rms * inv_rms * inner_mean)).astype(
        jnp.bfloat16
    )
    return (token_grad, weight_sum * grad_scale, gain_total * grad_scale)


def shards(tokens, norm_gain, key_weight, key_grad):
    n_rep, n_grp = lax.axis_size("rep"), lax.axis_size("grp")
    n_z = n_grp // 2
    if (
        n_rep == 2 * 2 and n_grp == 2 * 4
        and key_weight.shape[1] % (n_rep * LANES) == 0 and key_weight.shape[0] % 96 == 0
        and tokens.shape[1] % (18 * LANES) == 0 and tokens.shape[0] % LANES == 0
    ):
        return fused(n_rep, n_grp, tokens, norm_gain, key_weight, key_grad)
    return plain(tokens, norm_gain, key_weight, key_grad)


def solution(mesh):
    in_specs = (P(("rep", "grp"), None), P(), P("grp", None), P(("rep", "grp"), None))
    out_specs = (P(("rep", "grp"), None), P("grp", "rep"), P())
    return jax.shard_map(shards, mesh=mesh, in_specs=in_specs, out_specs=out_specs, check_vma=False)
```
